32 devices in a mesh: groups: 2 (over x), gz: 16 (over z, y, core).
Axes of the slice: x: 2, y: 2, z: 4, core: 2. Of those that a mesh axis runs over, the one named last changes fastest.
Arguments:
- labels: int32 [128, 256, 256], P(('groups', 'gz')), parts along dimension 0, may hold values from 0 to 7
- tensor_table: float32 [16, 7], P('groups'), parts along dimension 0, may hold values from -0.3 to 3.5, as said below
- bounds: float32 [4], P('groups'), parts along dimension 0, may hold values from 0 to 51, as said below
- right_side: float32 [128, 256, 256], P(('groups', 'gz')), parts along dimension 0, may hold values from -18 to 18
Outputs:
- solution: float32 [128, 256, 256], P(('groups', 'gz')), parts along dimension 0
- residual: float32 [128, 256, 256], P(('groups', 'gz')), parts along dimension 0
- residual_norm: float32 [2], P('groups'), parts along dimension 0
The draws below stay inside these ranges and needn't reach their ends.
There are 2 independent parts, one for each index of `groups`. The reference program is written for one: setup_inputs(seed, part) draws one part's arguments, and reference() takes and returns one part's arrays. A program takes and returns all parts, laid end to end along the dimension named above; each array names one. Nothing has to cross between parts.
Inputs may be any that keep to these rules, and one draw needn't show every extreme that they name: `tensor_table`: every tensor is diagonally dominant: each diagonal component exceeds the sum of the magnitudes of its row's off-diagonal components by 0.4 or more; reactions are positive. 0 < bounds[0] < bounds[1], and bounds[1] is at least the largest eigenvalue of the operator.
All inputs are finite; a program needn't handle non-finite values.
Results may differ from the reference program's by a relative error of at most 0.00002.
Values sent between devices are 32-bit elements; how exact they have to be, the bound alone decides.
No kernel may reach another device: no remote copies, remote signals or barrier semaphores. Data moves between devices by JAX's collectives and lax.ppermute only.
A program may use at most 256 MiB of HBM per device.

```python
import math
import jax
import jax.numpy as jnp

NY = 256
NZ = 256
ITERS = 3
PHASES = 8
NX = 64


def make_table(key):
    inner = jax.random.fold_in(key, 17)
    keys = jax.random.split(inner, 4)
    couplings = jax.random.uniform(keys[0], (PHASES, 3), jnp.float32, -0.3, 0.3)
    magnitude = jnp.abs(couplings)
    row_sums = jnp.stack([magnitude[:, 0] + magnitude[:, 1], magnitude[:, 0] + magnitude[:, 2], magnitude[:, 1] + magnitude[:, 2]], 1)
    excess = jnp.exp(jax.random.uniform(keys[1], (PHASES, 3), jnp.float32, math.log(0.5), math.log(2.5)))
    diagonal = 0.4 + row_sums + excess
    reaction = jnp.exp(jax.random.uniform(keys[2], (PHASES, 1), jnp.float32, math.log(0.005), math.log(0.05)))
    table = jnp.concatenate([diagonal, couplings, reaction], 1)
    return (table, couplings, diagonal - row_sums, reaction, keys[3])


def draw_tensor_table(key, part):
    table, couplings, axis_weights, reaction, spare = make_table(key)
    return table


def draw_bounds(key, part):
    table, couplings, axis_weights, reaction, spare = make_table(key)
    spare_keys = jax.random.split(spare, 2)
    positive = jnp.max(jnp.maximum(couplings, 0.0), 0)
    negative = jnp.max(jnp.maximum(-couplings, 0.0), 0)
    largest = jnp.sum(jnp.max(axis_weights, 0)) + jnp.sum(positive) + jnp.sum(negative)
    gershgorin = jnp.max(reaction) + 4.0 * largest
    upper = gershgorin * jax.random.uniform(spare_keys[0], (), jnp.float32, 1.0, 1.2)
    lower = upper * jnp.exp(jax.random.uniform(spare_keys[1], (), jnp.float32, math.log(0.02), math.log(0.1)))
    return jnp.stack([lower, upper]).astype(jnp.float32)


def draw_right_side(key, part):
    along = jnp.arange(NX, dtype=jnp.float32) / max(NX - 1, 1)
    along = along[:, None, None]
    noise = jnp.clip(jax.random.normal(key, (NX, NY, NZ), jnp.float32), -4.0, 4.0)
    return noise * (1.0 + 2.0 * along)


def plant(values, key, low, high):
    longest = values.shape.index(max(values.shape))
    spots = []
    for shift in (0, 1):
        where = [jax.random.randint(jax.random.fold_in(key, axis), (), 0, length) for axis, length in enumerate(values.shape)]
        where[longest] = (where[longest] + shift) % values.shape[longest]
        spots.append(tuple(where))
    return values.at[spots[0]].set(low).at[spots[1]].set(high)


def setup_inputs(seed: int = 0, part: int = 0) -> dict:
    streams_of = jax.random.split(jax.random.key(seed), 5)
    part_keys = jax.random.split(jax.random.fold_in(streams_of[4], part), 5)
    return {
        "labels": plant(jax.random.randint(part_keys[0], (NX, NY, NZ), 0, PHASES), jax.random.fold_in(part_keys[0], 1), 0, PHASES - 1).astype(jnp.int32),
        "tensor_table": draw_tensor_table(jax.random.fold_in(jax.random.fold_in(streams_of[4], part), 71), part),
        "bounds": draw_bounds(jax.random.fold_in(jax.random.fold_in(streams_of[4], part), 71), part),
        "right_side": draw_right_side(jax.random.fold_in(jax.random.fold_in(streams_of[4], part), 71), part),
    }


lattice_steps = ((1, 0, 0), (0, 1, 0), (0, 0, 1), (1, 1, 0), (1, -1, 0), (1, 0, 1), (1, 0, -1), (0, 1, 1), (0, 1, -1))

def phase_weights(tensor_table):
    k_xx = tensor_table[:, 0]
    k_yy = tensor_table[:, 1]
    k_zz = tensor_table[:, 2]
    k_xy = tensor_table[:, 3]
    k_xz = tensor_table[:, 4]
    k_yz = tensor_table[:, 5]
    weights = [k_xx - jnp.abs(k_xy) - jnp.abs(k_xz), k_yy - jnp.abs(k_xy) - jnp.abs(k_yz), k_zz - jnp.abs(k_xz) - jnp.abs(k_yz), jnp.maximum(k_xy, 0.0), jnp.maximum(-k_xy, 0.0), jnp.maximum(k_xz, 0.0), jnp.maximum(-k_xz, 0.0), jnp.maximum(k_yz, 0.0), jnp.maximum(-k_yz, 0.0)]
    return (weights, tensor_table[:, 6])

def cell_values(per_phase, labels):
    result = jnp.zeros(labels.shape, jnp.float32)
    for phase in range(per_phase.shape[0]):
        result = jnp.where(labels == phase, per_phase[phase], result)
    return result

def shifted(field, shift_x, shift_y, shift_z):
    length, rows, columns = field.shape
    padded = jnp.pad(field, ((0, 0), (1, 1), (1, 1)))
    return padded[1 + shift_x:length - 1 + shift_x, 1 + shift_y:1 + shift_y + rows, 1 + shift_z:1 + shift_z + columns]

def apply_operator(field, weights, reaction):
    middle_field = field[1:-1]
    image = reaction[1:-1] * middle_field
    for which, offset in enumerate(lattice_steps):
        own_weight = weights[which][1:-1]
        for direction_sign in (1, -1):
            step_x = direction_sign * offset[0]
            step_y = direction_sign * offset[1]
            step_z = direction_sign * offset[2]
            neighbour = shifted(field, step_x, step_y, step_z)
            link = 0.5 * (own_weight + shifted(weights[which], step_x, step_y, step_z))
            image = image + link * (middle_field - neighbour)
    return image

def pad_planes(field):
    return jnp.pad(field, ((1, 1), (0, 0), (0, 0)))

def reference(labels, tensor_table, bounds, right_side):
    per_phase, reaction_phase = phase_weights(tensor_table)
    weights = [pad_planes(cell_values(table_column, labels)) for table_column in per_phase]
    reaction = pad_planes(cell_values(reaction_phase, labels))
    lower_bound = bounds[0]
    upper_bound = bounds[1]
    centre = (upper_bound + lower_bound) / 2.0
    spread = (upper_bound - lower_bound) / 2.0
    sigma_ratio = centre / spread
    factor = 1.0 / sigma_ratio
    solution = jnp.zeros_like(right_side)
    residual = right_side
    direction = right_side / centre
    for iteration in range(ITERS):
        solution = solution + direction
        image = apply_operator(pad_planes(direction), weights, reaction)
        residual = residual - image
        new_factor = 1.0 / (2.0 * sigma_ratio - factor)
        direction = new_factor * factor * direction + 2.0 * new_factor / spread * residual
        factor = new_factor
    residual_norm = jnp.sqrt(jnp.sum(residual * residual)).reshape(1)
    return (solution, residual, residual_norm)
```

```python
import functools

import jax
import jax.numpy as jnp
from jax import lax
from jax.experimental import pallas as pl
from jax.experimental.pallas import tpu as pltpu
from jax.sharding import PartitionSpec as P

ITERS = 3
PHASES = 8
OUTSIDE = 8
BASE = 9
LANES = 128
SUB = 8
PAD = 8
HALO = 2

steps = (
    (1, 0, 0),
    (0, 1, 0),
    (0, 0, 1),
    (1, 1, 0),
    (1, -1, 0),
    (1, 0, 1),
    (1, 0, -1),
    (0, 1, 1),
    (0, 1, -1),
)
links = tuple((which, sign) for which in range(len(steps)) for sign in (1, -1))


def splat(value):
    return jnp.full((SUB, LANES), value, jnp.float32)


def look_up(table, index):
    return jnp.take_along_axis(table, index, axis=1, mode="promise_in_bounds")


def chebyshev(bounds_ref):
    lower, upper = splat(bounds_ref[0]), splat(bounds_ref[1])
    centre = (upper + lower) / 2.0
    half = (upper - lower) / 2.0
    sigma = centre / half
    rho = 1.0 / sigma
    factors = []
    for _ in range(ITERS):
        rho_new = 1.0 / (2.0 * sigma - rho)
        factors.append((rho_new * rho, 2.0 * rho_new / half))
        rho = rho_new
    return 1.0 / centre, factors


def link_tables(table_ref, flip):
    lane = lax.broadcasted_iota(jnp.int32, (SUB, LANES), 1)
    own, other = lane // BASE, lane % BASE
    turn = jnp.where(splat(flip.astype(jnp.float32)) > 0.5, -1.0, 1.0)
    columns = []
    for column in range(7):
        first = jnp.zeros((SUB, LANES), jnp.float32)
        second = jnp.zeros((SUB, LANES), jnp.float32)
        single = jnp.zeros((SUB, LANES), jnp.float32)
        for phase in range(PHASES):
            value = splat(table_ref[phase, column])
            first = jnp.where(own == phase, value, first)
            second = jnp.where(other == phase, value, second)
            single = jnp.where(lane == phase, value, single)
        if column in (3, 4):
            first, second = first * turn, second * turn
        columns.append((first, second, single))

    def weights(k):
        k_xx, k_yy, k_zz, k_xy, k_xz, k_yz = k
        return [
            k_xx - jnp.abs(k_xy) - jnp.abs(k_xz),
            k_yy - jnp.abs(k_xy) - jnp.abs(k_yz),
            k_zz - jnp.abs(k_xz) - jnp.abs(k_yz),
            jnp.maximum(k_xy, 0.0),
            jnp.maximum(-k_xy, 0.0),
            jnp.maximum(k_xz, 0.0),
            jnp.maximum(-k_xz, 0.0),
            jnp.maximum(k_yz, 0.0),
            jnp.maximum(-k_yz, 0.0),
        ]

    pairs = zip(weights([c[0] for c in columns[:6]]), weights([c[1] for c in columns[:6]]))
    return [0.5 * (a + b) for a, b in pairs], columns[6][2]


def put_lane_shifted(trio, plane, row, values, fill):
    lane = lax.broadcasted_iota(jnp.int32, (SUB, LANES), 1)
    count = len(values)
    up = [pltpu.roll(value, LANES - 1, 1) for value in values]
    down = [pltpu.roll(value, 1, 1) for value in values]
    edge = jnp.full((SUB, LANES), fill, values[0].dtype)
    for c in range(count):
        right = up[c + 1] if c + 1 < count else edge
        left = down[c - 1] if c else edge
        trio[0][plane, c, pl.ds(row + PAD, SUB), :] = values[c]
        trio[1][plane, c, pl.ds(row + PAD, SUB), :] = jnp.where(lane == LANES - 1, right, up[c])
        trio[2][plane, c, pl.ds(row + PAD, SUB), :] = jnp.where(lane == 0, left, down[c])


def fill_rims(trio, plane, tiles, rows, fill):
    edge = jnp.full((PAD, LANES), fill, trio[0].dtype)
    for ref in trio:
        for c in range(tiles):
            ref[plane, c, pl.ds(0, PAD), :] = edge
            ref[plane, c, pl.ds(rows + PAD, PAD), :] = edge


def neighbour(trio, plane, c, row, step):
    dx, dy, dz = step
    return trio[dz % 3][plane + dx, c, pl.ds(row + PAD + dy, SUB), :]


def signed(link):
    which, sign = link
    return tuple(sign * part for part in steps[which])


def each_block(rows, body, unroll=2):
    def step(k, carry):
        return body(pl.multiple_of(k * SUB, SUB), carry)

    return functools.partial(lax.fori_loop, 0, rows // SUB, step, unroll=unroll)


def set_labels(trio, plane, tiles, rows, read):
    fill_rims(trio, plane, tiles, rows, OUTSIDE)

    def body(row, carry):
        put_lane_shifted(trio, plane, row, [read(c, row) for c in range(tiles)], OUTSIDE)
        return carry

    each_block(rows, body)(0)


def set_links(labels, link_ref, plane, out, tiles, rows, tables, reaction):
    for c in range(tiles):

        def body(row, carry):
            mine = labels[0][plane, c, pl.ds(row + PAD, SUB), :]
            base = mine * BASE
            total = look_up(reaction, mine)
            for k, link in enumerate(links):
                value = look_up(tables[link[0]], base + neighbour(labels, plane, c, row, signed(link)))
                link_ref[out, k, c, pl.ds(row, SUB), :] = value
                total = total + value
            link_ref[out, len(links), c, pl.ds(row, SUB), :] = total
            return carry

        each_block(rows, body)(0)


def operator(field, link_ref, plane, at, c, row):
    where = pl.ds(row, SUB)
    parts = [link_ref[at, len(links), c, where, :] * neighbour(field, plane, c, row, (0, 0, 0))]
    sums = [None] * 3
    for k, link in enumerate(links):
        term = link_ref[at, k, c, where, :] * neighbour(field, plane, c, row, signed(link))
        sums[k % 3] = term if sums[k % 3] is None else sums[k % 3] + term
    return parts[0] - ((sums[0] + sums[1]) + sums[2])


def tile(ref, plane, c, row):
    return ref[plane, pl.ds(row, SUB), pl.ds(c * LANES, LANES)]


def inner_kernel(depth, labels_ref, right_ref, table_ref, bounds_ref, near_ref, far_ref, *scratch):
    labels, field, link_ref = scratch[:3], scratch[3:6], scratch[6]
    rows, tiles = labels_ref.shape[1], labels_ref.shape[2] // LANES
    flip = lax.axis_index("gz") % 2
    inverse, factors = chebyshev(bounds_ref)
    tables, reaction = link_tables(table_ref, flip)
    first, second = factors[0]

    for q in range(depth):
        source = jnp.where(flip == 1, depth - 1 - q, q)
        set_labels(labels, q, tiles, rows, lambda c, row: tile(labels_ref, source, c, row))
        fill_rims(field, q, tiles, rows, 0.0)

        def body(row, carry):
            values = [tile(right_ref, source, c, row) * inverse for c in range(tiles)]
            put_lane_shifted(field, q, row, values, 0.0)
            return carry

        each_block(rows, body)(0)

    for q, out in ((1, near_ref), (depth - 2, far_ref)):
        set_links(labels, link_ref, q, 0, tiles, rows, tables, reaction)
        source = jnp.where(flip == 1, depth - 1 - q, q)
        for c in range(tiles):

            def body(row, carry):
                rest = tile(right_ref, source, c, row) - operator(field, link_ref, q, 0, c, row)
                here = neighbour(field, q, c, row, (0, 0, 0))
                out[0, pl.ds(row, SUB), pl.ds(c * LANES, LANES)] = first * here + second * rest
                return carry

            each_block(rows, body)(0)


def main_kernel(
    depth,
    labels_ref,
    right_ref,
    table_ref,
    bounds_ref,
    labels_near_ref,
    right_near_ref,
    direction_near_ref,
    labels_far_ref,
    right_far_ref,
    direction_far_ref,
    solution_ref,
    residual_ref,
    squares_ref,
    *scratch,
):
    labels, field, link_ref, rest_ref = scratch[:3], scratch[3:6], scratch[6], scratch[7]
    rows, tiles = labels_ref.shape[1], labels_ref.shape[2] // LANES
    place, count = lax.axis_index("gz"), lax.axis_size("gz")
    flip = place % 2
    joined = jnp.logical_and(place > 0, place < count - 1)
    joined_mask = splat(joined.astype(jnp.float32))
    inverse, factors = chebyshev(bounds_ref)
    tables, reaction = link_tables(table_ref, flip)

    own = range(depth)
    inner_halo = (-1, depth)
    outer_halo = (-HALO, depth + 1)

    def source(q):
        if q in own:
            return labels_ref, right_ref, jnp.where(flip == 1, depth - 1 - q, q)
        far = q >= depth
        distance = q - depth if far else -1 - q
        order = distance == 0
        index = jnp.where(flip == (1 if far else 0), 1 if order else 0, 0 if order else 1)
        if far:
            return labels_far_ref, right_far_ref, index
        return labels_near_ref, right_near_ref, index

    for q in range(-HALO, depth + HALO):
        labels_from, right_from, index = source(q)

        def read(c, row):
            value = tile(labels_from, index, c, row)
            return jnp.where(joined, value, OUTSIDE) if q < 0 else value

        set_labels(labels, q + HALO, tiles, rows, read)
        fill_rims(field, q + HALO, tiles, rows, 0.0)

        def body(row, carry):
            values = [tile(right_from, index, c, row) * inverse for c in range(tiles)]
            put_lane_shifted(field, q + HALO, row, values, 0.0)
            return carry

        each_block(rows, body)(0)

    for q in range(-1, depth + 1):
        set_links(labels, link_ref, q + HALO, q + 1, tiles, rows, tables, reaction)

    for iteration in range(ITERS):
        last = iteration == ITERS - 1
        planes = own if last else range(-1, depth + 1)
        total = jnp.zeros((SUB, LANES), jnp.float32)
        for q in planes:
            _, right_from, index = source(q)
            for c in range(tiles):

                def body(row, carry):
                    image = operator(field, link_ref, q + HALO, q + 1, c, row)
                    if iteration == 0:
                        rest = tile(right_from, index, c, row) - image
                    else:
                        rest = rest_ref[q + 1, c, pl.ds(row, SUB), :] - image
                    if q < 0:
                        rest = rest * joined_mask
                    if last:
                        residual_ref[index, pl.ds(row, SUB), pl.ds(c * LANES, LANES)] = rest
                        return carry + rest * rest
                    rest_ref[q + 1, c, pl.ds(row, SUB), :] = rest
                    return carry

                total = each_block(rows, body)(total)
        if last:
            squares_ref[0, 0] = jnp.sum(total)
            break
        first, second = factors[iteration]
        for q in planes:
            _, _, index = source(q)

            def body(row, carry):
                values = []
                for c in range(tiles):
                    here = neighbour(field, q + HALO, c, row, (0, 0, 0))
                    value = first * here + second * rest_ref[q + 1, c, pl.ds(row, SUB), :]
                    values.append(value)
                    if q in own:
                        at = (index, pl.ds(row, SUB), pl.ds(c * LANES, LANES))
                        before = here if iteration == 0 else solution_ref[at]
                        solution_ref[at] = before + value
                put_lane_shifted(field, q + HALO, row, values, 0.0)
                return carry

            each_block(rows, body)(0)
        if iteration == 0:
            for q, received in zip(outer_halo, (direction_near_ref, direction_far_ref)):

                def body(row, carry):
                    put_lane_shifted(field, q + HALO, row, [tile(received, 0, c, row) for c in range(tiles)], 0.0)
                    return carry

                each_block(rows, body)(0)


def per_device(labels, tensor_table, bounds, right_side):
    depth, rows, columns = labels.shape
    tiles = columns // LANES
    count = lax.axis_size("gz")
    place = lax.axis_index("gz")
    odd = place % 2

    vmem = pl.BlockSpec(memory_space=pltpu.VMEM)
    smem = pl.BlockSpec(memory_space=pltpu.SMEM)

    def scratch(planes, linked):
        padded = (planes, tiles, rows + 2 * PAD, LANES)
        return (
            [pltpu.VMEM(padded, jnp.int32)] * 3
            + [pltpu.VMEM(padded, jnp.float32)] * 3
            + [pltpu.VMEM((linked, len(links) + 1, tiles, rows, LANES), jnp.float32)]
        )

    inside = [(i, i ^ 1) for i in range(count)]
    across = [(i, i + 1) for i in range(1, count - 1, 2)]
    across += [(j, i) for i, j in across]
    near_start = odd * (depth - HALO)
    far_start = (1 - odd) * (depth - HALO)

    def send(array, start, pairs):
        return lax.ppermute(lax.dynamic_slice_in_dim(array, start, HALO, 0), "gz", pairs)

    labels_near = send(labels, near_start, across)
    right_near = send(right_side, near_start, across)
    labels_far = send(labels, far_start, inside)
    right_far = send(right_side, far_start, inside)

    plane = jax.ShapeDtypeStruct((1, rows, columns), jnp.float32)
    near, far = pl.pallas_call(
        functools.partial(inner_kernel, depth),
        out_shape=(plane, plane),
        in_specs=[vmem, vmem, smem, smem],
        out_specs=(vmem, vmem),
        scratch_shapes=scratch(depth, 1),
        name="inner",
    )(labels, right_side, tensor_table, bounds)
    direction_near = lax.ppermute(near, "gz", across)
    direction_far = lax.ppermute(far, "gz", inside)

    block = jax.ShapeDtypeStruct(right_side.shape, jnp.float32)
    solved, residual, squares = pl.pallas_call(
        functools.partial(main_kernel, depth),
        out_shape=(block, block, jax.ShapeDtypeStruct((1, 1), jnp.float32)),
        in_specs=[vmem, vmem, smem, smem] + [vmem] * 6,
        out_specs=(vmem, vmem, smem),
        scratch_shapes=scratch(depth + 2 * HALO, depth + 2)
        + [pltpu.VMEM((depth + 2, tiles, rows, LANES), jnp.float32)],
        compiler_params=pltpu.CompilerParams(vmem_limit_bytes=60 * 1024 * 1024),
        name="main",
    )(
        labels,
        right_side,
        tensor_table,
        bounds,
        labels_near,
        right_near,
        direction_near,
        labels_far,
        right_far,
        direction_far,
    )
    gathered = lax.all_to_all(jnp.broadcast_to(squares.reshape(1), (count,)), "gz", 0, 0, tiled=True)
    return solved, residual, jnp.sqrt(jnp.sum(gathered)).reshape(1)


def solution(mesh):
    whole = P(("groups", "gz"), None, None)
    return jax.shard_map(
        per_device,
        mesh=mesh,
        in_specs=(whole, P("groups", None), P("groups"), whole),
        out_specs=(whole, whole, P("groups")),
        check_vma=False,
    )
```

```python
import functools

import jax
import jax.numpy as jnp
from jax import lax
from jax.experimental import pallas as pl
from jax.experimental.pallas import tpu as pltpu
from jax.sharding import PartitionSpec as P

ITERS = 3
PHASES = 8
LANES = 128
SUB = 8
PAD = 8
BELOW = 8
RIM = 16
RIM_BELOW = 24
HALO = 2

steps = (
    (1, 0, 0),
    (0, 1, 0),
    (0, 0, 1),
    (1, 1, 0),
    (1, -1, 0),
    (1, 0, 1),
    (1, 0, -1),
    (0, 1, 1),
    (0, 1, -1),
)
cross = [d for d, step in enumerate(steps) if step[0]]
inplane = [d for d, step in enumerate(steps) if not step[0]]
sideways = [d for d, step in enumerate(steps) if step[2]]


def slots(directions):
    order = [(d, 0) for d in directions] + [(d, 1) for d in directions if steps[d][2]]
    return {key: k for k, key in enumerate(order)}


cross_slots, inplane_slots = slots(cross), slots(inplane)


def splat(value):
    return jnp.full((SUB, LANES), value, jnp.float32)


def chebyshev(bounds_ref):
    lower, upper = splat(bounds_ref[0]), splat(bounds_ref[1])
    centre = (upper + lower) / 2.0
    half = (upper - lower) / 2.0
    sigma = centre / half
    rho = 1.0 / sigma
    factors = []
    for _ in range(ITERS):
        rho_new = 1.0 / (2.0 * sigma - rho)
        factors.append((rho_new * rho, 2.0 * rho_new / half))
        rho = rho_new
    return 1.0 / centre, factors


def each_block(rows, body, carry=0, unroll=8):
    count = rows // SUB

    def step(k, carry):
        return body(pl.multiple_of(k * SUB, SUB), carry)

    carry = lax.fori_loop(0, count - count % unroll, step, carry, unroll=unroll)
    for k in range(count - count % unroll, count):
        carry = body(k * SUB, carry)
    return carry


def lane_shifted(values, dz, edge):
    lane = lax.broadcasted_iota(jnp.int32, (SUB, LANES), 1)
    turned = [pltpu.roll(value, LANES - 1 if dz == 1 else 1, 1) for value in values]
    if dz == 1:
        beyond = turned[1:] + [edge]
        return [jnp.where(lane == LANES - 1, b, t) for t, b in zip(turned, beyond)]
    beyond = [edge] + turned[:-1]
    return [jnp.where(lane == 0, b, t) for t, b in zip(turned, beyond)]


def put_field(field, plane, row, values):
    zero = splat(0.0)
    for variant, dz in ((0, 0), (1, 1), (2, -1)):
        shifted = lane_shifted(values, dz, zero) if dz else values
        for c, value in enumerate(shifted):
            field[plane, c, variant, pl.ds(row + PAD, SUB), :] = value


def field_rims(field, plane, tiles, rows):
    for variant in range(3):
        for c in range(tiles):
            field[plane, c, variant, pl.ds(0, PAD), :] = splat(0.0)
            field[plane, c, variant, pl.ds(rows + PAD, PAD), :] = splat(0.0)


def tile(ref, plane, c, row):
    return ref[plane, pl.ds(row, SUB), pl.ds(c * LANES, LANES)]


def put_tile(ref, plane, c, row, value):
    ref[plane, pl.ds(row, SUB), pl.ds(c * LANES, LANES)] = value


class Half:
    def __init__(self, table_ref, flip, refs, tiles, rows):
        self.refs, self.tiles, self.rows = refs, tiles, rows
        turn = jnp.where(splat(flip.astype(jnp.float32)) > 0.5, -0.5, 0.5)
        self.tables = []
        for phase in range(PHASES):
            k = [splat(table_ref[phase, column]) for column in range(7)]
            size = [jnp.abs(value) for value in k]
            self.tables.append(
                (
                    (0.5 * (k[0] - size[3] - size[4]), turn * k[3], turn * k[4]),
                    (0.5 * (k[1] - size[3] - size[5]), 0.5 * (k[2] - size[4] - size[5]), 0.5 * k[5], k[6]),
                )
            )
        for ref, slots_of in zip(refs, (cross_slots, inplane_slots)):
            for slot in range(ref.shape[0]):
                for k in range(len(slots_of)):
                    for c in range(tiles):
                        for start in (0, SUB, rows + RIM, rows + RIM + SUB):
                            ref[slot, c, k, pl.ds(start, SUB), :] = splat(0.0)

    def fill(self, slot, read, mask=None, reaction=None):
        for group in range(2 if reaction else 1):
            tables = [t[group] for t in self.tables]
            if mask is not None:
                tables = [[mask * value for value in t] for t in tables]
            ref, at = (self.refs[1], 0) if group else (self.refs[0], slot)
            places = inplane_slots if group else cross_slots

            def body(row, carry):
                found = {}
                for c in range(self.tiles):
                    label = read(c, row)
                    bits = [(label & (1 << b)) != 0 for b in range(3)]
                    looked = []
                    for column in range(len(tables[0])):
                        level = [t[column] for t in tables]
                        for bit in bits:
                            level = [jnp.where(bit, b, a) for a, b in zip(level[::2], level[1::2])]
                        looked.append(level[0])
                    if group == 0:
                        values = {0: looked[0]}
                        signed = zip((3, 5), looked[1:])
                    else:
                        values = {1: looked[0], 2: looked[1]}
                        signed = [(7, looked[2])]
                        reaction[0][reaction[1], c, pl.ds(row, SUB), :] = looked[3]
                    for d, value in signed:
                        values[d] = jnp.maximum(value, 0.0)
                        values[d + 1] = jnp.maximum(-value, 0.0)
                    for d, value in values.items():
                        ref[at, c, places[d, 0], pl.ds(row + RIM, SUB), :] = value
                        found.setdefault(d, []).append(value)
                for d, values in found.items():
                    if steps[d][2]:
                        for c, value in enumerate(lane_shifted(values, steps[d][2], splat(0.0))):
                            ref[at, c, places[d, 1], pl.ds(row + RIM, SUB), :] = value
                return carry

            each_block(self.rows, body)

    def link(self, slot, other, out, at):
        directions, places = (cross, cross_slots) if other is not None else (inplane, inplane_slots)
        ref = self.refs[0 if other is not None else 1]
        slot, other = (slot, other) if other is not None else (0, 0)

        def body(row, carry):
            for d in directions:
                dx, dy, dz = steps[d]
                near = pl.ds(row + RIM - PAD, SUB)
                far = pl.ds(row + RIM - PAD + dy, SUB)
                ahead = [ref[other, c, places[d, 1 if dz else 0], far, :] for c in range(self.tiles)]
                values = [ref[slot, c, places[d, 0], near, :] + ahead[c] for c in range(self.tiles)]
                for c, value in enumerate(values):
                    out[at, c, places[d, 0], pl.ds(row, SUB), :] = value
                if dz:
                    edge = ref[other, 0 if dz == 1 else self.tiles - 1, places[d, 0], far, :]
                    for c, value in enumerate(lane_shifted(values, -dz, edge)):
                        out[at, c, places[d, 1], pl.ds(row, SUB), :] = value
            return carry

        each_block(self.rows + 2 * PAD, body)


def apply_operator(field, cross_ref, inplane_ref, reaction_ref, planes, tiles, rows, use):
    for c in range(tiles):

        def body(row, carry):
            held = {}

            def value(q, dy, dz):
                key = (q, dy, dz)
                if key not in held:
                    held[key] = field[q + HALO, c, dz % 3, pl.ds(row + PAD + dy, SUB), :]
                return held[key]

            for q in planes:
                here = value(q, 0, 0)
                image = reaction_ref[q + 1, c, pl.ds(row, SUB), :] * here
                sums = [image, None, None]
                k = 0
                for d, (dx, dy, dz) in enumerate(steps):
                    places = cross_slots if dx else inplane_slots
                    ref, base = (cross_ref, HALO) if dx else (inplane_ref, 1)
                    for sign in (1, -1):
                        if sign == 1:
                            link = ref[q + base, c, places[d, 0], pl.ds(row + PAD, SUB), :]
                        else:
                            key = places[d, 1 if dz else 0]
                            link = ref[q + base - dx, c, key, pl.ds(row + PAD - dy, SUB), :]
                        term = link * (here - value(q + sign * dx, sign * dy, sign * dz))
                        sums[k % 3] = term if sums[k % 3] is None else sums[k % 3] + term
                        k += 1
                carry = use(q, c, row, sums[0] + (sums[1] + sums[2]), here, carry)
            return carry

        yield body


def run_operator(*arguments, carry=0):
    rows = arguments[6]
    for body in apply_operator(*arguments):
        carry = each_block(rows, body, carry, unroll=4)
    return carry


class Device:
    def __init__(self, shape):
        self.depth, self.rows, self.tiles = shape[0], shape[1], shape[2] // LANES
        self.place, self.count = lax.axis_index("gz"), lax.axis_size("gz")
        self.flip = self.place % 2
        joined = jnp.logical_and(self.place > 0, self.place < self.count - 1)
        self.joined = splat(joined.astype(jnp.float32))

    def own(self, q):
        return jnp.where(self.flip == 1, self.depth - 1 - q, q)

    def halo(self, q):
        far = q >= self.depth
        first = (q == self.depth) if far else (q == -1)
        turned = self.flip == (1 if far else 0)
        return jnp.where(turned, 1, 0) if first else jnp.where(turned, 0, 1)


def start_kernel(labels_hbm, right_hbm, table_ref, bounds_ref, *refs):
    labels_ref, first_ref, cross_ref, inplane_ref, reaction_ref, rest_ref, near_ref, far_ref = refs[:8]
    right_ref, sems, *halves = refs[8:]
    copies = [
        pltpu.make_async_copy(source, target, sems.at[k])
        for k, (source, target) in enumerate(((right_hbm, right_ref), (labels_hbm, labels_ref)))
    ]
    for copy in copies:
        copy.start()
    device = Device(labels_ref.shape)
    depth, rows, tiles = device.depth, device.rows, device.tiles
    inverse, factors = chebyshev(bounds_ref)
    half = Half(table_ref, device.flip, halves, tiles, rows)
    copies[0].wait()
    for q in range(depth):
        index = device.own(q)
        field_rims(first_ref, q + HALO, tiles, rows)

        def body(row, carry):
            values = [tile(right_ref, index, c, row) for c in range(tiles)]
            for c, value in enumerate(values):
                rest_ref[q + 1, c, pl.ds(row, SUB), :] = value
            put_field(first_ref, q + HALO, row, [value * inverse for value in values])
            return carry

        each_block(rows, body)
    copies[1].wait()
    for q in range(depth):
        index = device.own(q)
        half.fill(q % 2, lambda c, row: tile(labels_ref, index, c, row), None, (reaction_ref, q + 1))
        if q:
            half.link((q - 1) % 2, q % 2, cross_ref, q - 1 + HALO)
        half.link(q % 2, None, inplane_ref, q + 1)

    ahead, behind = factors[0]

    def use(q, c, row, image, here, carry):
        rest = rest_ref[q + 1, c, pl.ds(row, SUB), :] - image
        rest_ref[q + 1, c, pl.ds(row, SUB), :] = rest
        for plane, out in ((1, near_ref), (depth - 2, far_ref)):
            if q == plane:
                put_tile(out, 0, c, row, ahead * here + behind * rest)
        return carry

    run_operator(first_ref, cross_ref, inplane_ref, reaction_ref, range(1, depth - 1), tiles, rows, use)


def halo_links(device, half, labels_ref, near_labels_ref, far_labels_ref, cross_ref, inplane_ref, reaction_ref):
    depth = device.depth

    def own(q):
        index = device.own(q)
        return lambda c, row: tile(labels_ref, index, c, row)

    def halo(ref, q):
        index = device.halo(q)
        return lambda c, row: tile(ref, index, c, row)

    for inner, outer, furthest, ref in ((depth - 1, depth, depth + 1, far_labels_ref), (0, -1, -2, near_labels_ref)):
        mask = device.joined if outer < 0 else None
        half.fill(0, own(inner))
        half.fill(1, halo(ref, outer), mask, (reaction_ref, outer + 1))
        half.link(1, None, inplane_ref, outer + 1)
        if outer > 0:
            half.link(0, 1, cross_ref, inner + HALO)
            half.fill(0, halo(ref, furthest), mask)
            half.link(1, 0, cross_ref, outer + HALO)
        else:
            half.link(1, 0, cross_ref, outer + HALO)
            half.fill(0, halo(ref, furthest), mask)
            half.link(0, 1, cross_ref, furthest + HALO)


class Solve:
    def __init__(self, device, refs, factors, right):
        self.device, self.refs, self.factors, self.right = device, refs, factors, right

    def subtract(self, iteration, planes, last=None):
        device = self.device
        first_ref, second_ref, cross_ref, inplane_ref, reaction_ref, rest_ref, _ = self.refs
        field = second_ref if iteration == 1 else first_ref

        def use(q, c, row, image, here, carry):
            if iteration == 0 and not 0 <= q < device.depth:
                rest = self.right(q, c, row) - image
            else:
                rest = rest_ref[q + 1, c, pl.ds(row, SUB), :] - image
            if q < 0:
                rest = rest * device.joined
            rest_ref[q + 1, c, pl.ds(row, SUB), :] = rest
            return carry

        run_operator(
            field, cross_ref, inplane_ref, reaction_ref, planes, device.tiles, device.rows, last or use
        )

    def direct(self, iteration, planes):
        device = self.device
        first_ref, second_ref, _, _, _, rest_ref, sum_ref = self.refs
        old, new = (first_ref, second_ref) if iteration == 0 else (second_ref, first_ref)
        ahead, behind = self.factors[iteration]
        for q in planes:
            if iteration == 0:
                field_rims(new, q + HALO, device.tiles, device.rows)

            def body(row, carry):
                values = []
                for c in range(device.tiles):
                    here = old[q + HALO, c, 0, pl.ds(row + PAD, SUB), :]
                    value = ahead * here + behind * rest_ref[q + 1, c, pl.ds(row, SUB), :]
                    values.append(value)
                    if 0 <= q < device.depth:
                        before = here if iteration == 0 else sum_ref[q, c, pl.ds(row, SUB), :]
                        sum_ref[q, c, pl.ds(row, SUB), :] = before + value
                put_field(new, q + HALO, row, values)
                return carry

            each_block(device.rows, body)

    def receive(self, field, q, read):
        field_rims(field, q + HALO, self.device.tiles, self.device.rows)

        def body(row, carry):
            put_field(field, q + HALO, row, [read(c, row) for c in range(self.device.tiles)])
            return carry

        each_block(self.device.rows, body)


def middle_kernel(*refs):
    _, _, _, _, _, labels_ref, table_ref, bounds_ref = refs[:8]
    far_labels_ref, far_right_ref, far_second_ref, near_labels_ref = refs[8:12]
    first_ref, cross_ref, inplane_ref, reaction_ref, rest_ref, second_ref, sum_ref, *halves = refs[12:]
    device = Device(labels_ref.shape)
    depth = device.depth
    inverse, factors = chebyshev(bounds_ref)
    half = Half(table_ref, device.flip, halves, device.tiles, device.rows)
    halo_links(device, half, labels_ref, near_labels_ref, far_labels_ref, cross_ref, inplane_ref, reaction_ref)

    def right(q, c, row):
        return tile(far_right_ref, device.halo(q), c, row)

    solve = Solve(
        device, (first_ref, second_ref, cross_ref, inplane_ref, reaction_ref, rest_ref, sum_ref), factors, right
    )
    for q in (depth, depth + 1):
        index = device.halo(q)
        solve.receive(first_ref, q, lambda c, row: tile(far_right_ref, index, c, row) * inverse)
    solve.subtract(0, [depth - 1, depth])
    solve.direct(0, range(1, depth + 1))
    solve.receive(second_ref, depth + 1, lambda c, row: tile(far_second_ref, 0, c, row))
    solve.subtract(1, range(2, depth + 1))
    solve.direct(1, range(2, depth + 1))
    solve.subtract(2, range(3, depth))


def last_kernel(
    first_in,
    second_in,
    rest_in,
    sum_in,
    cross_ref,
    inplane_ref,
    reaction_ref,
    bounds_ref,
    near_right_ref,
    near_second_ref,
    first_ref,
    second_ref,
    rest_ref,
    sum_ref,
    solution_ref,
    residual_ref,
    squares_ref,
):
    device = Device(residual_ref.shape)
    depth, rows, tiles = device.depth, device.rows, device.tiles
    inverse, factors = chebyshev(bounds_ref)

    def right(q, c, row):
        return tile(near_right_ref, device.halo(q), c, row)

    refs = (first_ref, second_ref, cross_ref, inplane_ref, reaction_ref, rest_ref, sum_ref)
    solve = Solve(device, refs, factors, right)
    for q in (-1, -2):
        index = device.halo(q)
        solve.receive(first_ref, q, lambda c, row: tile(near_right_ref, index, c, row) * inverse)
    solve.subtract(0, [-1, 0])
    solve.direct(0, [-1, 0])
    solve.receive(second_ref, -2, lambda c, row: tile(near_second_ref, 0, c, row))
    solve.subtract(1, [-1, 0, 1])
    solve.direct(1, [-1, 0, 1])

    def use(q, c, row, image, here, carry):
        rest = rest_ref[q + 1, c, pl.ds(row, SUB), :] - image
        put_tile(residual_ref, device.own(q), c, row, rest)
        return carry + rest * rest

    planes = range(0, min(3, depth))
    total = run_operator(
        first_ref, cross_ref, inplane_ref, reaction_ref, planes, tiles, rows, use, carry=splat(0.0)
    )
    for c in range(tiles):

        def body(row, carry):
            for q in range(3, depth):
                rest = rest_ref[q + 1, c, pl.ds(row, SUB), :]
                put_tile(residual_ref, device.own(q), c, row, rest)
                carry = carry + rest * rest
            for q in range(depth):
                put_tile(solution_ref, device.own(q), c, row, sum_ref[q, c, pl.ds(row, SUB), :])
            return carry

        total = each_block(rows, body, total)
    squares_ref[...] = jnp.broadcast_to(jnp.sum(total), squares_ref.shape)


def per_device(labels, tensor_table, bounds, right_side):
    depth, rows, columns = labels.shape
    tiles = columns // LANES
    count = lax.axis_size("gz")
    odd = lax.axis_index("gz") % 2

    vmem = pl.BlockSpec(memory_space=pltpu.VMEM)
    smem = pl.BlockSpec(memory_space=pltpu.SMEM)
    hbm = pl.BlockSpec(memory_space=pltpu.HBM)

    def array(*shape):
        return jax.ShapeDtypeStruct(shape, jnp.float32)

    below = rows + PAD + BELOW
    first = array(depth + 2 * HALO, tiles, 3, below, LANES)
    cross_links = array(depth + 2 * HALO - 1, tiles, len(cross_slots), below, LANES)
    inplane_links = array(depth + 2, tiles, len(inplane_slots), below, LANES)
    reaction = array(depth + 2, tiles, rows, LANES)
    total = array(depth, tiles, rows, LANES)
    plane = array(1, rows, columns)
    halves = [
        pltpu.VMEM((count_, tiles, len(places), rows + RIM + RIM_BELOW, LANES), jnp.float32)
        for count_, places in ((2, cross_slots), (1, inplane_slots))
    ]

    def call(kernel, name, out_shape, in_specs, aliases, limit, cycles, scratch=()):
        return pl.pallas_call(
            kernel,
            out_shape=out_shape,
            in_specs=in_specs,
            out_specs=[vmem] * len(out_shape),
            scratch_shapes=list(scratch),
            input_output_aliases=aliases,
            compiler_params=pltpu.CompilerParams(vmem_limit_bytes=limit),
            cost_estimate=pl.CostEstimate(flops=cycles, bytes_accessed=1 << 20, transcendentals=0),
            name=name,
        )

    inside = [(i, i ^ 1) for i in range(count)]
    across = [(i, i + 1) for i in range(1, count - 1, 2)]
    across += [(j, i) for i, j in across]
    near_start = odd * (depth - HALO)
    far_start = (1 - odd) * (depth - HALO)

    def send(name, array, start, pairs):
        with jax.named_scope(name):
            return lax.ppermute(lax.dynamic_slice_in_dim(array, start, HALO, 0), "gz", pairs)

    near_labels = send("near_labels", labels, near_start, across)
    near_right = send("near_right", right_side, near_start, across)
    far_labels = send("far_labels", labels, far_start, inside)
    far_right = send("far_right", right_side, far_start, inside)

    state = (first, cross_links, inplane_links, reaction, reaction)
    own_labels, *state, near, far = call(
        start_kernel,
        "start",
        (jax.ShapeDtypeStruct(labels.shape, jnp.int32),) + state + (plane, plane),
        [hbm, hbm, smem, smem],
        {},
        9 << 20,
        10**8,
        [pltpu.VMEM(right_side.shape, jnp.float32), pltpu.SemaphoreType.DMA((2,))] + halves,
    )(labels, right_side, tensor_table, bounds)
    with jax.named_scope("near_second"):
        near_second = lax.ppermute(near, "gz", across)
    with jax.named_scope("far_second"):
        far_second = lax.ppermute(far, "gz", inside)

    outs = call(
        middle_kernel,
        "middle",
        tuple(array(*s.shape) for s in state) + (first, total),
        [vmem] * 6 + [smem, smem] + [vmem] * 4,
        {k: k for k in range(5)},
        7 << 20,
        10**8,
        halves,
    )(*state, own_labels, tensor_table, bounds, far_labels, far_right, far_second, near_labels)
    first, cross_links, inplane_links, reaction, rest, second, total = outs

    *_, solved, residual, squares = call(
        last_kernel,
        "last",
        tuple(array(*s.shape) for s in (first, second, rest, total))
        + (array(*right_side.shape), array(*right_side.shape), array(count, LANES)),
        [vmem] * 7 + [smem] + [vmem] * 2,
        {k: k for k in range(4)},
        6 << 20,
        10**8,
    )(first, second, rest, total, cross_links, inplane_links, reaction, bounds, near_right, near_second)
    gathered = lax.all_to_all(squares, "gz", 0, 0, tiled=True)
    return solved, residual, jnp.sqrt(jnp.sum(gathered[:, 0])).reshape(1)


def solution(mesh):
    whole = P(("groups", "gz"), None, None)
    return jax.shard_map(
        per_device,
        mesh=mesh,
        in_specs=(whole, P("groups", None), P("groups"), whole),
        out_specs=(whole, whole, P("groups")),
        check_vma=False,
    )
```

```python
import jax
import jax.numpy as jnp
from jax import lax
from jax.experimental import pallas as pl
from jax.experimental.pallas import tpu as pltpu
from jax.sharding import PartitionSpec as P


ITERS = 3
PHASES = 8
LANES = 128
SUB = 8
PAD = 8
BELOW = 8
RIM = 16
RIM_BELOW = 24
HALO = 2
LIMITS = (8, 8, 5, 5)

steps = (
    (1, 0, 0),
    (0, 1, 0),
    (0, 0, 1),
    (1, 1, 0),
    (1, -1, 0),
    (1, 0, 1),
    (1, 0, -1),
    (0, 1, 1),
    (0, 1, -1),
)
cross = [d for d, step in enumerate(steps) if step[0]]
inplane = [d for d, step in enumerate(steps) if not step[0]]


def slots(directions):
    order = [(d, 0) for d in directions] + [(d, 1) for d in directions if steps[d][2]]
    return {key: k for k, key in enumerate(order)}


cross_slots, inplane_slots = slots(cross), slots(inplane)


def splat(value):
    return jnp.full((SUB, LANES), value, jnp.float32)


def chebyshev(bounds_ref):
    lower, upper = splat(bounds_ref[0]), splat(bounds_ref[1])
    centre = (upper + lower) / 2.0
    half = (upper - lower) / 2.0
    sigma = centre / half
    rho = 1.0 / sigma
    factors = []
    for _ in range(ITERS):
        rho_new = 1.0 / (2.0 * sigma - rho)
        factors.append((rho_new * rho, 2.0 * rho_new / half))
        rho = rho_new
    return 1.0 / centre, factors


def each_block(rows, body, carry=0, unroll=None):
    count = rows // SUB
    unroll = min(unroll or 16, count)

    def step(k, carry):
        return body(pl.multiple_of(k * SUB, SUB), carry)

    carry = lax.fori_loop(0, count - count % unroll, step, carry, unroll=unroll)
    for k in range(count - count % unroll, count):
        carry = body(k * SUB, carry)
    return carry


def lane_shifted(values, dz, edge):
    lane = lax.broadcasted_iota(jnp.int32, (SUB, LANES), 1)
    turned = [pltpu.roll(value, LANES - 1 if dz == 1 else 1, 1) for value in values]
    if dz == 1:
        beyond = turned[1:] + [edge]
        return [jnp.where(lane == LANES - 1, b, t) for t, b in zip(turned, beyond)]
    beyond = [edge] + turned[:-1]
    return [jnp.where(lane == 0, b, t) for t, b in zip(turned, beyond)]


def put_field(field, plane, row, values):
    zero = splat(0.0)
    for variant, dz in ((0, 0), (1, 1), (2, -1)):
        shifted = lane_shifted(values, dz, zero) if dz else values
        for c, value in enumerate(shifted):
            field[plane, c, variant, pl.ds(row + PAD, SUB), :] = value


def field_rims(field, plane, tiles, rows):
    for variant in range(3):
        for c in range(tiles):
            field[plane, c, variant, pl.ds(0, PAD), :] = splat(0.0)
            field[plane, c, variant, pl.ds(rows + PAD, PAD), :] = splat(0.0)


def tile(ref, plane, c, row):
    return ref[plane, pl.ds(row, SUB), pl.ds(c * LANES, LANES)]


def put_tile(ref, plane, c, row, value):
    ref[plane, pl.ds(row, SUB), pl.ds(c * LANES, LANES)] = value


def put_tables(tables_ref, table_ref, flip):
    turn = jnp.where(splat(flip.astype(jnp.float32)) > 0.5, -0.5, 0.5)
    for phase in range(PHASES):
        k = [splat(table_ref[phase, column]) for column in range(7)]
        size = [jnp.abs(value) for value in k]
        values = (
            0.5 * (k[0] - size[3] - size[4]),
            turn * k[3],
            turn * k[4],
            0.5 * (k[1] - size[3] - size[5]),
            0.5 * (k[2] - size[4] - size[5]),
            0.5 * k[5],
            k[6],
        )
        for place, value in enumerate(values):
            tables_ref[phase, place] = value


def put_factors(factors_ref, bounds_ref):
    inverse, factors = chebyshev(bounds_ref)
    for k, value in enumerate([inverse] + [value for pair in factors for value in pair]):
        factors_ref[k] = value


def get_factors(factors_ref):
    pairs = [(factors_ref[1 + 2 * k], factors_ref[2 + 2 * k]) for k in range(ITERS)]
    return factors_ref[0], pairs


class Half:
    def __init__(self, tables_ref, refs, tiles, rows):
        self.refs, self.tiles, self.rows = refs, tiles, rows
        self.tables = [
            ([tables_ref[phase, k] for k in range(3)], [tables_ref[phase, k] for k in range(3, 7)])
            for phase in range(PHASES)
        ]
        for ref, slots_of in zip(refs, (cross_slots, inplane_slots)):
            for slot in range(ref.shape[0]):
                for k in range(len(slots_of)):
                    for c in range(tiles):
                        for start in (0, SUB, rows + RIM, rows + RIM + SUB):
                            ref[slot, c, k, pl.ds(start, SUB), :] = splat(0.0)

    def fill(self, slot, read, mask=None, reaction=None):
        for group in range(2 if reaction else 1):
            tables = [t[group] for t in self.tables]
            if mask is not None:
                tables = [[mask * value for value in t] for t in tables]
            ref, at = (self.refs[1], 0) if group else (self.refs[0], slot)
            places = inplane_slots if group else cross_slots

            def body(row, carry):
                found = {}
                for c in range(self.tiles):
                    label = read(c, row)
                    bits = [(label & (1 << b)) != 0 for b in range(3)]
                    looked = []
                    for column in range(len(tables[0])):
                        level = [t[column] for t in tables]
                        for bit in bits:
                            level = [jnp.where(bit, b, a) for a, b in zip(level[::2], level[1::2])]
                        looked.append(level[0])
                    if group == 0:
                        values = {0: looked[0]}
                        signed = zip((3, 5), looked[1:])
                    else:
                        values = {1: looked[0], 2: looked[1]}
                        signed = [(7, looked[2])]
                        reaction[0][reaction[1], c, pl.ds(row, SUB), :] = looked[3]
                    for d, value in signed:
                        values[d] = jnp.maximum(value, 0.0)
                        values[d + 1] = jnp.maximum(-value, 0.0)
                    for d, value in values.items():
                        ref[at, c, places[d, 0], pl.ds(row + RIM, SUB), :] = value
                        found.setdefault(d, []).append(value)
                for d, values in found.items():
                    if steps[d][2]:
                        for c, value in enumerate(lane_shifted(values, steps[d][2], splat(0.0))):
                            ref[at, c, places[d, 1], pl.ds(row + RIM, SUB), :] = value
                return carry

            each_block(self.rows, body)

    def link(self, slot, other, out, at):
        directions, places = (cross, cross_slots) if other is not None else (inplane, inplane_slots)
        ref = self.refs[0 if other is not None else 1]
        slot, other = (slot, other) if other is not None else (0, 0)

        def body(row, carry):
            for d in directions:
                _, dy, dz = steps[d]
                near = pl.ds(row + RIM - PAD, SUB)
                far = pl.ds(row + RIM - PAD + dy, SUB)
                ahead = [ref[other, c, places[d, 1 if dz else 0], far, :] for c in range(self.tiles)]
                values = [ref[slot, c, places[d, 0], near, :] + ahead[c] for c in range(self.tiles)]
                for c, value in enumerate(values):
                    out[at, c, places[d, 0], pl.ds(row, SUB), :] = value
                if dz:
                    edge = ref[other, 0 if dz == 1 else self.tiles - 1, places[d, 0], far, :]
                    for c, value in enumerate(lane_shifted(values, -dz, edge)):
                        out[at, c, places[d, 1], pl.ds(row, SUB), :] = value
            return carry

        each_block(self.rows + 2 * PAD, body)


def apply_operator(field, cross_ref, inplane_ref, reaction_ref, planes, tiles, rows, use, parts=None):
    whole = (-1, 0, 1)
    for c in range(tiles):

        def body(row, carry):
            held = {}

            def value(q, dy, dz):
                key = (q, dy, dz)
                if key not in held:
                    held[key] = field[q + HALO, c, dz % 3, pl.ds(row + PAD + dy, SUB), :]
                return held[key]

            for q in planes:
                here = value(q, 0, 0)
                wanted = (parts or {}).get(q, whole)
                sums = [reaction_ref[q + 1, c, pl.ds(row, SUB), :] * here] if 0 in wanted else []
                for d, (dx, dy, dz) in enumerate(steps):
                    places = cross_slots if dx else inplane_slots
                    ref, base = (cross_ref, HALO) if dx else (inplane_ref, 1)
                    for sign in (1, -1):
                        if sign * dx not in wanted:
                            continue
                        if sign == 1:
                            link = ref[q + base, c, places[d, 0], pl.ds(row + PAD, SUB), :]
                        else:
                            key = places[d, 1 if dz else 0]
                            link = ref[q + base - dx, c, key, pl.ds(row + PAD - dy, SUB), :]
                        term = link * (here - value(q + sign * dx, sign * dy, sign * dz))
                        sums = sums[1:] + [sums[0] + term] if len(sums) == 3 else sums + [term]
                carry = use(q, c, row, sums[0] + (sums[1] + sums[2]), here, carry)
            return carry

        yield body


def run_operator(*arguments, carry=0):
    rows = arguments[6]
    for body in apply_operator(*arguments):
        carry = each_block(rows, body, carry, unroll=4)
    return carry


class Device:
    def __init__(self, shape):
        self.depth, self.rows, self.tiles = shape[0], shape[1], shape[2] // LANES
        self.place, self.count = lax.axis_index("gz"), lax.axis_size("gz")
        self.flip = self.place % 2
        joined = jnp.logical_and(self.place > 0, self.place < self.count - 1)
        self.joined = splat(joined.astype(jnp.float32))

    def own(self, q):
        return jnp.where(self.flip == 1, self.depth - 1 - q, q)

    def sent(self, q):
        return jnp.where(self.flip == 1, 1 - q % HALO, q % HALO)

    def halo(self, q):
        far = q >= self.depth
        first = (q == self.depth) if far else (q == -1)
        turned = self.flip == (1 if far else 0)
        return jnp.where(turned, 1, 0) if first else jnp.where(turned, 0, 1)


class Solve:
    def __init__(self, device, refs, factors, right=None):
        self.device, self.refs, self.factors, self.right = device, refs, factors, right

    def subtract(self, iteration, planes, parts=None):
        device = self.device
        first_ref, second_ref, cross_ref, inplane_ref, reaction_ref, rest_ref, _ = self.refs
        field = second_ref if iteration == 1 else first_ref

        def use(q, c, row, image, here, carry):
            if iteration == 0 and not 0 <= q < device.depth:
                rest = self.right(q, c, row) - image
            else:
                rest = rest_ref[q + 1, c, pl.ds(row, SUB), :] - image
            if q < 0:
                rest = rest * device.joined
            rest_ref[q + 1, c, pl.ds(row, SUB), :] = rest
            return carry

        run_operator(
            field, cross_ref, inplane_ref, reaction_ref, planes, device.tiles, device.rows, use, parts
        )

    def direct(self, iteration, planes, copies={}):
        device = self.device
        first_ref, second_ref, _, _, _, rest_ref, sum_ref = self.refs
        old, new = (first_ref, second_ref) if iteration == 0 else (second_ref, first_ref)
        ahead, behind = self.factors[iteration]
        for q in planes:
            if q < 0:
                field_rims(new, q + HALO, device.tiles, device.rows)

            def body(row, carry):
                values = []
                for c in range(device.tiles):
                    here = old[q + HALO, c, 0, pl.ds(row + PAD, SUB), :]
                    value = ahead * here + behind * rest_ref[q + 1, c, pl.ds(row, SUB), :]
                    values.append(value)
                    if q in copies:
                        put_tile(copies[q], 0, c, row, value)
                    if 0 <= q < device.depth and sum_ref is not None:
                        before = here if iteration == 0 else sum_ref[q, c, pl.ds(row, SUB), :]
                        sum_ref[q, c, pl.ds(row, SUB), :] = before + value
                put_field(new, q + HALO, row, values)
                return carry

            each_block(device.rows, body)

    def receive(self, field, q, read):
        field_rims(field, q + HALO, self.device.tiles, self.device.rows)

        def body(row, carry):
            put_field(field, q + HALO, row, [read(c, row) for c in range(self.device.tiles)])
            return carry

        each_block(self.device.rows, body)


def start_kernel(*refs):
    near_labels_ref, near_right_ref, far_labels_ref, far_right_ref, beside_labels_ref, beside_right_ref = refs[:6]
    table_ref, bounds_ref, tables_ref, factors_ref = refs[6:10]
    first_ref, cross_ref, inplane_ref, reaction_ref, rest_ref, second_ref, sum_ref, near_ref, far_ref = refs[10:19]
    halves = refs[19:]
    device = Device((2 * HALO,) + near_labels_ref.shape[1:])
    depth, rows, tiles = device.depth, device.rows, device.tiles
    put_factors(factors_ref, bounds_ref)
    inverse, factors = get_factors(factors_ref)
    put_tables(tables_ref, table_ref, device.flip)
    half = Half(tables_ref, halves, tiles, rows)

    def read(q, near, far, beside):
        if q == depth:
            ref, index = beside, device.halo(q)
        else:
            ref, index = near if q < HALO else far, device.sent(q)
        return lambda c, row: tile(ref, index, c, row)

    for q in range(depth + 1):
        field_rims(first_ref, q + HALO, tiles, rows)
        field_rims(second_ref, q + HALO, tiles, rows)
        right = read(q, near_right_ref, far_right_ref, beside_right_ref)

        def body(row, carry):
            values = [right(c, row) for c in range(tiles)]
            if q < depth:
                for c, value in enumerate(values):
                    rest_ref[q + 1, c, pl.ds(row, SUB), :] = value
            put_field(first_ref, q + HALO, row, [value * inverse for value in values])
            return carry

        each_block(rows, body)
        labels = read(q, near_labels_ref, far_labels_ref, beside_labels_ref)
        half.fill(q % 2, labels, None, (reaction_ref, q + 1) if q < depth else None)
        if q:
            half.link((q - 1) % 2, q % 2, cross_ref, q - 1 + HALO)
        if q < depth:
            half.link(q % 2, None, inplane_ref, q + 1)

    solve = Solve(device, (first_ref, second_ref, cross_ref, inplane_ref, reaction_ref, rest_ref, sum_ref), factors)
    solve.subtract(0, range(1, depth))
    solve.direct(0, range(1, depth), {1: near_ref, depth - 1: far_ref})


def middle_kernel(*refs):
    tables_ref, factors_ref, sent_labels_ref, far_second_ref, near_labels_ref = refs[7:12]
    first_ref, cross_ref, inplane_ref, reaction_ref, rest_ref, second_ref, sum_ref, far_ref, *halves = refs[12:]
    device = Device((2 * HALO,) + near_labels_ref.shape[1:])
    depth = device.depth
    _, factors = get_factors(factors_ref)
    solve = Solve(device, (first_ref, second_ref, cross_ref, inplane_ref, reaction_ref, rest_ref, sum_ref), factors)
    solve.receive(second_ref, depth, lambda c, row: tile(far_second_ref, 0, c, row))
    solve.subtract(1, range(2, depth))
    solve.direct(1, range(2, depth), {depth - 1: far_ref})

    def labels(ref, index):
        return lambda c, row: tile(ref, index, c, row)

    half = Half(tables_ref, halves, device.tiles, device.rows)
    half.fill(0, labels(sent_labels_ref, device.sent(0)))
    half.fill(1, labels(near_labels_ref, device.halo(-1)), device.joined, (reaction_ref, 0))
    half.link(1, None, inplane_ref, 0)
    half.link(1, 0, cross_ref, HALO - 1)
    half.fill(0, labels(near_labels_ref, device.halo(-2)), device.joined)
    half.link(0, 1, cross_ref, HALO - 2)


def late_kernel(*refs):
    cross_ref, inplane_ref, reaction_ref, factors_ref, near_right_ref = refs[4:9]
    first_ref, second_ref, rest_ref, sum_ref, solution_ref = refs[9:]
    device = Device(solution_ref.shape)
    depth = device.depth
    inverse, factors = get_factors(factors_ref)

    def right(q, c, row):
        return tile(near_right_ref, device.halo(q), c, row)

    solve = Solve(
        device, (first_ref, second_ref, cross_ref, inplane_ref, reaction_ref, rest_ref, sum_ref), factors, right
    )
    for q in (-1, -2):
        index = device.halo(q)
        solve.receive(first_ref, q, lambda c, row: tile(near_right_ref, index, c, row) * inverse)
    solve.subtract(0, [-1, 0])
    solve.direct(0, [-1, 0])
    solve.subtract(1, [-1, 0, 1], parts={-1: (0, 1)})
    solve.direct(1, [0, 1])
    solve.subtract(2, range(depth), parts={0: (0, 1), depth - 1: (-1, 0)})
    for c in range(device.tiles):

        def body(row, carry):
            for q in range(depth):
                put_tile(solution_ref, device.own(q), c, row, sum_ref[q, c, pl.ds(row, SUB), :])
            return carry

        each_block(device.rows, body)


def last_kernel(*refs):
    cross_ref, inplane_ref, reaction_ref, factors_ref, near_second_ref, far_third_ref = refs[3:9]
    first_ref, second_ref, rest_ref, residual_ref, squares_ref = refs[9:]
    device = Device(residual_ref.shape)
    depth, rows, tiles = device.depth, device.rows, device.tiles
    _, factors = get_factors(factors_ref)
    solve = Solve(device, (first_ref, second_ref, cross_ref, inplane_ref, reaction_ref, rest_ref, None), factors)
    solve.receive(first_ref, depth, lambda c, row: tile(far_third_ref, 0, c, row))
    solve.receive(second_ref, -2, lambda c, row: tile(near_second_ref, 0, c, row))
    solve.subtract(1, [-1], parts={-1: (-1,)})
    solve.direct(1, [-1])

    def use(q, c, row, image, here, carry):
        for plane in [0] + list(range(1, depth - 1)) if q == 0 else [q]:
            rest = rest_ref[plane + 1, c, pl.ds(row, SUB), :]
            if plane == q:
                rest = rest - image
            put_tile(residual_ref, device.own(plane), c, row, rest)
            carry = carry + rest * rest
        return carry

    total = run_operator(
        first_ref,
        cross_ref,
        inplane_ref,
        reaction_ref,
        [0, depth - 1],
        tiles,
        rows,
        use,
        {0: (-1,), depth - 1: (1,)},
        carry=splat(0.0),
    )
    squares_ref[...] = jnp.broadcast_to(jnp.sum(total), squares_ref.shape)


def per_device(labels, tensor_table, bounds, right_side):
    depth, rows, columns = labels.shape
    if depth != 2 * HALO or columns % LANES or rows % SUB:
        raise ValueError("unsupported block")
    tiles = columns // LANES
    count = lax.axis_size("gz")
    odd = lax.axis_index("gz") % 2

    vmem = pl.BlockSpec(memory_space=pltpu.VMEM)
    smem = pl.BlockSpec(memory_space=pltpu.SMEM)

    def array(*shape):
        return jax.ShapeDtypeStruct(shape, jnp.float32)

    below = rows + PAD + BELOW
    field = array(depth + HALO + 1, tiles, 3, below, LANES)
    cross_links = array(depth + HALO, tiles, len(cross_slots), below, LANES)
    inplane_links = array(depth + 1, tiles, len(inplane_slots), below, LANES)
    reaction = rest = array(depth + 1, tiles, rows, LANES)
    total = array(depth, tiles, rows, LANES)
    plane = array(1, rows, columns)
    block = array(depth, rows, columns)
    tables, factors = array(PHASES, 7, SUB, LANES), array(1 + 2 * ITERS, SUB, LANES)
    halves = [
        pltpu.VMEM((planes, tiles, len(places), rows + RIM + RIM_BELOW, LANES), jnp.float32)
        for planes, places in ((2, cross_slots), (1, inplane_slots))
    ]

    def call(kernel, arguments, out_shape, aliased, limit, flops, scratch=(), scalars=0):
        return pl.pallas_call(
            kernel,
            out_shape=out_shape,
            in_specs=[vmem] * (len(arguments) - scalars) + [smem] * scalars,
            out_specs=[vmem] * len(out_shape),
            scratch_shapes=list(scratch),
            input_output_aliases={k: k for k in range(aliased)},
            compiler_params=pltpu.CompilerParams(vmem_limit_bytes=limit << 20),
            cost_estimate=pl.CostEstimate(flops=flops, bytes_accessed=1 << 20, transcendentals=0),
        )(*arguments)

    inside = [(i, i ^ 1) for i in range(count)]
    across = [(i, i + 1) for i in range(1, count - 1, 2)]
    across += [(j, i) for i, j in across]
    near_start = odd * (depth - HALO)
    far_start = (1 - odd) * (depth - HALO)

    def send(array, pairs):
        return lax.ppermute(array, "gz", pairs)

    def ends(array):
        return [lax.dynamic_slice_in_dim(array, start, HALO, 0) for start in (near_start, far_start)]

    my_labels, my_right = ends(labels), ends(right_side)
    near_labels = send(my_labels[0], across)
    near_right = send(my_right[0], across)
    far_labels = send(my_labels[1], inside)
    far_right = send(my_right[1], inside)

    tables, factors, *state, near, far = call(
        start_kernel,
        (my_labels[0], my_right[0], my_labels[1], my_right[1], far_labels, far_right, tensor_table, bounds),
        (tables, factors, field, cross_links, inplane_links, reaction, rest, field, total, plane, plane),
        0,
        LIMITS[0],
        10**8,
        halves,
        scalars=2,
    )
    near_second = send(near, across)
    far_second = send(far, inside)

    *state, far = call(
        middle_kernel,
        (*state, tables, factors, my_labels[0], far_second, near_labels),
        tuple(array(*s.shape) for s in state) + (plane,),
        7,
        LIMITS[1],
        10**8,
        halves,
    )
    far_third = send(far, inside)
    first, cross_links, inplane_links, reaction, rest, second, total = state
    links = (cross_links, inplane_links, reaction, factors)
    first, second, rest, _, solved = call(
        late_kernel,
        (first, second, rest, total, *links, near_right),
        (field, field, array(*rest.shape), array(*total.shape), block),
        4,
        LIMITS[2],
        10**8,
    )
    *_, residual, squares = call(
        last_kernel,
        (first, second, rest, *links, near_second, far_third),
        (field, field, array(*rest.shape), block, array(count, LANES)),
        3,
        LIMITS[3],
        10**8,
    )
    gathered = lax.all_to_all(squares, "gz", 0, 0, tiled=True)
    return solved, residual, jnp.sqrt(jnp.sum(gathered[:, 0])).reshape(1)


def solution(mesh):
    whole = P(("groups", "gz"), None, None)
    return jax.shard_map(
        per_device,
        mesh=mesh,
        in_specs=(whole, P("groups", None), P("groups"), whole),
        out_specs=(whole, whole, P("groups")),
        check_vma=False,
    )
```

```python
import jax
import jax.numpy as jnp
from jax import lax
from jax.experimental import pallas as pl
from jax.experimental.pallas import tpu as pltpu
from jax.sharding import PartitionSpec as P


ITERS = 3
PHASES = 8
LANES = 128
SUB = 8
PAD = 8
BELOW = 8
RIM = 16
RIM_BELOW = 24
HALO = 2
OPERATOR_UNROLL = 8
LIMITS = (8, 8, 5, 5)

steps = (
    (1, 0, 0),
    (0, 1, 0),
    (0, 0, 1),
    (1, 1, 0),
    (1, -1, 0),
    (1, 0, 1),
    (1, 0, -1),
    (0, 1, 1),
    (0, 1, -1),
)
cross = [d for d, step in enumerate(steps) if step[0]]
inplane = [d for d, step in enumerate(steps) if not step[0]]


def slots(directions):
    order = [(d, 0) for d in directions] + [(d, 1) for d in directions if steps[d][2]]
    return {key: k for k, key in enumerate(order)}


cross_slots, inplane_slots = slots(cross), slots(inplane)


def splat(value):
    return jnp.full((SUB, LANES), value, jnp.float32)


def chebyshev(bounds_ref):
    lower, upper = splat(bounds_ref[0]), splat(bounds_ref[1])
    centre = (upper + lower) / 2.0
    half = (upper - lower) / 2.0
    sigma = centre / half
    rho = 1.0 / sigma
    factors = []
    for _ in range(ITERS):
        rho_new = 1.0 / (2.0 * sigma - rho)
        factors.append((rho_new * rho, 2.0 * rho_new / half))
        rho = rho_new
    return 1.0 / centre, factors


def each_block(rows, body, carry=0, unroll=None):
    count = rows // SUB
    unroll = min(unroll or 16, count)

    def step(k, carry):
        return body(pl.multiple_of(k * SUB, SUB), carry)

    carry = lax.fori_loop(0, count - count % unroll, step, carry, unroll=unroll)
    for k in range(count - count % unroll, count):
        carry = body(k * SUB, carry)
    return carry


def lane_shifted(values, dz, edge):
    lane = lax.broadcasted_iota(jnp.int32, (SUB, LANES), 1)
    turned = [pltpu.roll(value, LANES - 1 if dz == 1 else 1, 1) for value in values]
    if dz == 1:
        beyond = turned[1:] + [edge]
        return [jnp.where(lane == LANES - 1, b, t) for t, b in zip(turned, beyond)]
    beyond = [edge] + turned[:-1]
    return [jnp.where(lane == 0, b, t) for t, b in zip(turned, beyond)]


def put_field(field, plane, row, values):
    zero = splat(0.0)
    for variant, dz in ((0, 0), (1, 1), (2, -1)):
        shifted = lane_shifted(values, dz, zero) if dz else values
        for c, value in enumerate(shifted):
            field[plane, c, variant, pl.ds(row + PAD, SUB), :] = value


def field_rims(field, plane, tiles, rows):
    for variant in range(3):
        for c in range(tiles):
            field[plane, c, variant, pl.ds(0, PAD), :] = splat(0.0)
            field[plane, c, variant, pl.ds(rows + PAD, PAD), :] = splat(0.0)


def tile(ref, plane, c, row):
    return ref[plane, pl.ds(row, SUB), pl.ds(c * LANES, LANES)]


def put_tile(ref, plane, c, row, value):
    ref[plane, pl.ds(row, SUB), pl.ds(c * LANES, LANES)] = value


def put_tables(tables_ref, table_ref, flip):
    turn = jnp.where(splat(flip.astype(jnp.float32)) > 0.5, -0.5, 0.5)
    for phase in range(PHASES):
        k = [splat(table_ref[phase, column]) for column in range(7)]
        size = [jnp.abs(value) for value in k]
        values = (
            0.5 * (k[0] - size[3] - size[4]),
            turn * k[3],
            turn * k[4],
            0.5 * (k[1] - size[3] - size[5]),
            0.5 * (k[2] - size[4] - size[5]),
            0.5 * k[5],
            k[6],
        )
        for place, value in enumerate(values):
            tables_ref[phase, place] = value


def put_factors(factors_ref, bounds_ref):
    inverse, factors = chebyshev(bounds_ref)
    for k, value in enumerate([inverse] + [value for pair in factors for value in pair]):
        factors_ref[k] = value


def get_factors(factors_ref):
    pairs = [(factors_ref[1 + 2 * k], factors_ref[2 + 2 * k]) for k in range(ITERS)]
    return factors_ref[0], pairs


class Half:
    def __init__(self, tables_ref, refs, tiles, rows):
        self.refs, self.tiles, self.rows = refs, tiles, rows
        self.tables = [
            ([tables_ref[phase, k] for k in range(3)], [tables_ref[phase, k] for k in range(3, 7)])
            for phase in range(PHASES)
        ]
        for ref, slots_of in zip(refs, (cross_slots, inplane_slots)):
            for slot in range(ref.shape[0]):
                for k in range(len(slots_of)):
                    for c in range(tiles):
                        for start in (0, SUB, rows + RIM, rows + RIM + SUB):
                            ref[slot, c, k, pl.ds(start, SUB), :] = splat(0.0)

    def fill(self, slot, read, mask=None, reaction=None):
        for group in range(2 if reaction else 1):
            tables = [t[group] for t in self.tables]
            if mask is not None:
                tables = [[mask * value for value in t] for t in tables]
            ref, at = (self.refs[1], 0) if group else (self.refs[0], slot)
            places = inplane_slots if group else cross_slots

            def body(row, carry):
                found = {}
                for c in range(self.tiles):
                    label = read(c, row)
                    bits = [(label & (1 << b)) != 0 for b in range(3)]
                    looked = []
                    for column in range(len(tables[0])):
                        level = [t[column] for t in tables]
                        for bit in bits:
                            level = [jnp.where(bit, b, a) for a, b in zip(level[::2], level[1::2])]
                        looked.append(level[0])
                    if group == 0:
                        values = {0: looked[0]}
                        signed = zip((3, 5), looked[1:])
                    else:
                        values = {1: looked[0], 2: looked[1]}
                        signed = [(7, looked[2])]
                        reaction[0][reaction[1], c, pl.ds(row, SUB), :] = looked[3]
                    for d, value in signed:
                        values[d] = jnp.maximum(value, 0.0)
                        values[d + 1] = jnp.maximum(-value, 0.0)
                    for d, value in values.items():
                        ref[at, c, places[d, 0], pl.ds(row + RIM, SUB), :] = value
                        found.setdefault(d, []).append(value)
                for d, values in found.items():
                    if steps[d][2]:
                        for c, value in enumerate(lane_shifted(values, steps[d][2], splat(0.0))):
                            ref[at, c, places[d, 1], pl.ds(row + RIM, SUB), :] = value
                return carry

            each_block(self.rows, body)

    def link(self, slot, other, out, at):
        directions, places = (cross, cross_slots) if other is not None else (inplane, inplane_slots)
        ref = self.refs[0 if other is not None else 1]
        slot, other = (slot, other) if other is not None else (0, 0)

        def body(row, carry):
            for d in directions:
                _, dy, dz = steps[d]
                near = pl.ds(row + RIM - PAD, SUB)
                far = pl.ds(row + RIM - PAD + dy, SUB)
                ahead = [ref[other, c, places[d, 1 if dz else 0], far, :] for c in range(self.tiles)]
                values = [ref[slot, c, places[d, 0], near, :] + ahead[c] for c in range(self.tiles)]
                for c, value in enumerate(values):
                    out[at, c, places[d, 0], pl.ds(row, SUB), :] = value
                if dz:
                    edge = ref[other, 0 if dz == 1 else self.tiles - 1, places[d, 0], far, :]
                    for c, value in enumerate(lane_shifted(values, -dz, edge)):
                        out[at, c, places[d, 1], pl.ds(row, SUB), :] = value
            return carry

        each_block(self.rows + 2 * PAD, body, unroll=17)


def run_operator(field, links, planes, device, use, parts={}, carry=0):
    cross_ref, inplane_ref, reaction_ref = links

    def body(row, carry):
        held = {}

        def value(q, c, dy, dz):
            key = (q, c, dy, dz)
            if key not in held:
                held[key] = field[q + HALO, c, dz % 3, pl.ds(row + PAD + dy, SUB), :]
            return held[key]

        def image(q, c):
            here = value(q, c, 0, 0)
            wanted = parts.get(q, (-1, 0, 1))
            sums = [reaction_ref[q + 1, c, pl.ds(row, SUB), :] * here] if 0 in wanted else []
            for d, (dx, dy, dz) in enumerate(steps):
                places = cross_slots if dx else inplane_slots
                ref, base = (cross_ref, HALO) if dx else (inplane_ref, 1)
                for sign in (1, -1):
                    if sign * dx not in wanted:
                        continue
                    if sign == 1:
                        link = ref[q + base, c, places[d, 0], pl.ds(row + PAD, SUB), :]
                    else:
                        key = places[d, 1 if dz else 0]
                        link = ref[q + base - dx, c, key, pl.ds(row + PAD - dy, SUB), :]
                    term = link * (here - value(q + sign * dx, c, sign * dy, sign * dz))
                    sums = sums[1:] + [sums[0] + term] if len(sums) == 3 else sums + [term]
            return sums[0] + (sums[1] + sums[2])

        for q in planes:
            images = [image(q, c) for c in range(device.tiles)]
            carry = use(q, row, images, [value(q, c, 0, 0) for c in range(device.tiles)], carry)
        return carry

    return each_block(device.rows, body, carry, unroll=OPERATOR_UNROLL)


class Device:
    def __init__(self, shape):
        self.depth, self.rows, self.tiles = shape[0], shape[1], shape[2] // LANES
        self.place, self.count = lax.axis_index("gz"), lax.axis_size("gz")
        self.flip = self.place % 2
        joined = jnp.logical_and(self.place > 0, self.place < self.count - 1)
        self.joined = splat(joined.astype(jnp.float32))

    def own(self, q):
        return jnp.where(self.flip == 1, self.depth - 1 - q, q)

    def sent(self, q):
        return jnp.where(self.flip == 1, 1 - q % HALO, q % HALO)

    def halo(self, q):
        far = q >= self.depth
        first = (q == self.depth) if far else (q == -1)
        turned = self.flip == (1 if far else 0)
        return jnp.where(turned, 1, 0) if first else jnp.where(turned, 0, 1)


class Solve:
    def __init__(self, device, refs, factors, right=None):
        self.device, self.factors, self.right = device, factors, right
        self.first, self.second, *self.links, self.rest = refs

    def advance(self, iteration, planes, direct=(), parts={}, copies={}, keep=None):
        device, rest_ref = self.device, self.rest
        old, new = (self.first, self.second) if iteration == 0 else (self.second, self.first)
        ahead, behind = self.factors[iteration]
        if iteration == 2:
            old, new = new, old
        for q in direct:
            if q < 0:
                field_rims(new, q + HALO, device.tiles, device.rows)

        def use(q, row, images, here, carry):
            block = pl.ds(row, SUB)
            if self.right and iteration == 0 and q < 0:
                before = [self.right(q, c, row) for c in range(device.tiles)]
            else:
                before = [rest_ref[q + 1, c, block, :] for c in range(device.tiles)]
            rest = [b - image for b, image in zip(before, images)]
            if q < 0:
                rest = [device.joined * r for r in rest]
            for c, r in enumerate(rest):
                rest_ref[q + 1, c, block, :] = r
            if q in direct:
                values = [ahead * h + behind * r for h, r in zip(here, rest)]
                if q in copies:
                    for c, v in enumerate(values):
                        put_tile(copies[q], 0, c, row, v)
                if keep and 0 <= q:
                    for c, (h, v) in enumerate(zip(here, values)):
                        keep(q, c, row, new[q + HALO, c, 0, pl.ds(row + PAD, SUB), :] + h + v)
                put_field(new, q + HALO, row, values)
            return carry

        run_operator(old, self.links, planes, device, use, parts)

    def receive(self, field, q, read):
        field_rims(field, q + HALO, self.device.tiles, self.device.rows)

        def body(row, carry):
            put_field(field, q + HALO, row, [read(c, row) for c in range(self.device.tiles)])
            return carry

        each_block(self.device.rows, body)


def start_kernel(*refs):
    near_labels_ref, near_right_ref, far_labels_ref, far_right_ref, beside_labels_ref, beside_right_ref = refs[:6]
    table_ref, bounds_ref, tables_ref, factors_ref = refs[6:10]
    first_ref, cross_ref, inplane_ref, reaction_ref, rest_ref, second_ref, near_ref, far_ref = refs[10:18]
    halves = refs[18:]
    device = Device((2 * HALO,) + near_labels_ref.shape[1:])
    depth, rows, tiles = device.depth, device.rows, device.tiles
    put_factors(factors_ref, bounds_ref)
    inverse, factors = get_factors(factors_ref)
    put_tables(tables_ref, table_ref, device.flip)
    half = Half(tables_ref, halves, tiles, rows)

    def read(q, near, far, beside):
        if q == depth:
            ref, index = beside, device.halo(q)
        else:
            ref, index = near if q < HALO else far, device.sent(q)
        return lambda c, row: tile(ref, index, c, row)

    for q in range(depth + 1):
        field_rims(first_ref, q + HALO, tiles, rows)
        field_rims(second_ref, q + HALO, tiles, rows)
        right = read(q, near_right_ref, far_right_ref, beside_right_ref)

        def body(row, carry):
            values = [right(c, row) for c in range(tiles)]
            if q < depth:
                for c, value in enumerate(values):
                    rest_ref[q + 1, c, pl.ds(row, SUB), :] = value
            put_field(first_ref, q + HALO, row, [value * inverse for value in values])
            return carry

        each_block(rows, body)
        labels = read(q, near_labels_ref, far_labels_ref, beside_labels_ref)
        half.fill(q % 2, labels, None, (reaction_ref, q + 1) if q < depth else None)
        if q:
            half.link((q - 1) % 2, q % 2, cross_ref, q - 1 + HALO)
        if q < depth:
            half.link(q % 2, None, inplane_ref, q + 1)

    solve = Solve(device, (first_ref, second_ref, cross_ref, inplane_ref, reaction_ref, rest_ref), factors)
    solve.advance(0, range(1, depth), range(1, depth), copies={1: near_ref, depth - 1: far_ref})


def middle_kernel(*refs):
    tables_ref, factors_ref, sent_labels_ref, far_second_ref, near_labels_ref = refs[6:11]
    first_ref, cross_ref, inplane_ref, reaction_ref, rest_ref, second_ref, far_ref, sum_ref, *halves = refs[11:]
    device = Device((2 * HALO,) + near_labels_ref.shape[1:])
    depth = device.depth
    _, factors = get_factors(factors_ref)
    solve = Solve(device, (first_ref, second_ref, cross_ref, inplane_ref, reaction_ref, rest_ref), factors)
    solve.receive(second_ref, depth, lambda c, row: tile(far_second_ref, 0, c, row))

    def keep(q, c, row, value):
        put_tile(sum_ref, q - HALO, c, row, value)

    solve.advance(1, range(HALO, depth), range(HALO, depth), copies={depth - 1: far_ref}, keep=keep)

    def labels(ref, index):
        return lambda c, row: tile(ref, index, c, row)

    half = Half(tables_ref, halves, device.tiles, device.rows)
    half.fill(0, labels(sent_labels_ref, device.sent(0)))
    half.fill(1, labels(near_labels_ref, device.halo(-1)), device.joined, (reaction_ref, 0))
    half.link(1, None, inplane_ref, 0)
    half.link(1, 0, cross_ref, HALO - 1)
    half.fill(0, labels(near_labels_ref, device.halo(-2)), device.joined)
    half.link(0, 1, cross_ref, HALO - 2)


def late_kernel(*refs):
    *links, factors_ref, near_right_ref, sum_ref = refs[3:9]
    first_ref, second_ref, rest_ref, solution_ref, ready_ref, sems = refs[9:]
    device = Device(solution_ref.shape)
    depth = device.depth
    inverse, factors = get_factors(factors_ref)
    copies = [
        pltpu.make_async_copy(
            ready_ref.at[q] if q < HALO else sum_ref.at[q - HALO], solution_ref.at[device.own(q)], sems.at[q]
        )
        for q in range(depth)
    ]
    for copy in copies[HALO:]:
        copy.start()

    def right(q, c, row):
        return tile(near_right_ref, device.halo(q), c, row)

    def keep(q, c, row, value):
        put_tile(ready_ref, q, c, row, value)

    solve = Solve(device, (first_ref, second_ref, *links, rest_ref), factors, right)
    for q in (-1, -2):
        index = device.halo(q)
        solve.receive(first_ref, q, lambda c, row: tile(near_right_ref, index, c, row) * inverse)
    solve.advance(0, [-1, 0], [-1, 0])
    solve.advance(1, [-1, 0, 1], [0, 1], parts={-1: (0, 1)}, keep=keep)
    for copy in copies[:HALO]:
        copy.start()
    solve.advance(2, range(depth), parts={0: (0, 1), depth - 1: (-1, 0)})
    for copy in copies:
        copy.wait()


def last_kernel(*refs):
    *links, factors_ref, near_second_ref, far_third_ref = refs[3:9]
    first_ref, second_ref, rest_ref, residual_ref, squares_ref, sems = refs[9:]
    device = Device(residual_ref.shape)
    depth = device.depth
    copies = {
        q: [
            pltpu.make_async_copy(
                rest_ref.at[q + 1, c],
                residual_ref.at[device.own(q), :, pl.ds(c * LANES, LANES)],
                sems.at[q, c],
            )
            for c in range(device.tiles)
        ]
        for q in range(depth)
    }
    for q in range(1, depth - 1):
        for copy in copies[q]:
            copy.start()
    _, factors = get_factors(factors_ref)
    solve = Solve(device, (first_ref, second_ref, *links, rest_ref), factors)
    solve.receive(first_ref, depth, lambda c, row: tile(far_third_ref, 0, c, row))
    solve.receive(second_ref, -2, lambda c, row: tile(near_second_ref, 0, c, row))
    solve.advance(1, [-1], [-1], parts={-1: (-1,)})

    def use(q, row, images, here, carry):
        for c, image in enumerate(images):
            for plane in range(depth - 1) if q == 0 else [q]:
                rest = rest_ref[plane + 1, c, pl.ds(row, SUB), :]
                if plane == q:
                    rest = rest - image
                    rest_ref[plane + 1, c, pl.ds(row, SUB), :] = rest
                carry = carry + rest * rest
        return carry

    ends = {0: (-1,), depth - 1: (1,)}
    total = run_operator(first_ref, links, list(ends), device, use, ends, splat(0.0))
    for q in ends:
        for copy in copies[q]:
            copy.start()
    squares_ref[...] = jnp.broadcast_to(jnp.sum(total), squares_ref.shape)
    for q in range(depth):
        for copy in copies[q]:
            copy.wait()


def per_device(labels, tensor_table, bounds, right_side):
    depth, rows, columns = labels.shape
    if depth != 2 * HALO or columns % LANES or rows % SUB:
        raise ValueError("unsupported block")
    tiles = columns // LANES
    count = lax.axis_size("gz")
    odd = lax.axis_index("gz") % 2

    vmem = pl.BlockSpec(memory_space=pltpu.VMEM)
    smem = pl.BlockSpec(memory_space=pltpu.SMEM)
    hbm = pl.BlockSpec(memory_space=pltpu.HBM)

    def array(*shape):
        return jax.ShapeDtypeStruct(shape, jnp.float32)

    below = rows + PAD + BELOW
    field = array(depth + HALO + 1, tiles, 3, below, LANES)
    cross_links = array(depth + HALO, tiles, len(cross_slots), below, LANES)
    inplane_links = array(depth + 1, tiles, len(inplane_slots), below, LANES)
    reaction = rest = array(depth + 1, tiles, rows, LANES)
    inner = array(depth - HALO, rows, columns)
    plane = array(1, rows, columns)
    block = array(depth, rows, columns)
    tables, factors = array(PHASES, 7, SUB, LANES), array(1 + 2 * ITERS, SUB, LANES)
    halves = [
        pltpu.VMEM((planes, tiles, len(places), rows + RIM + RIM_BELOW, LANES), jnp.float32)
        for planes, places in ((2, cross_slots), (1, inplane_slots))
    ]

    def call(kernel, arguments, out_shape, aliased, limit, flops, scratch=(), smem_count=0, kept=None):
        return pl.pallas_call(
            kernel,
            out_shape=out_shape,
            in_specs=[vmem] * (len(arguments) - smem_count) + [smem] * smem_count,
            out_specs=[hbm if k == kept else vmem for k in range(len(out_shape))],
            scratch_shapes=list(scratch),
            input_output_aliases={k: k for k in range(aliased)},
            compiler_params=pltpu.CompilerParams(vmem_limit_bytes=limit << 20),
            cost_estimate=pl.CostEstimate(flops=flops, bytes_accessed=1 << 20, transcendentals=0),
        )(*arguments)

    inside = [(i, i ^ 1) for i in range(count)]
    across = [(i, i + 1) for i in range(1, count - 1, 2)]
    across += [(j, i) for i, j in across]
    near_start = odd * (depth - HALO)
    far_start = (1 - odd) * (depth - HALO)

    def send(array, pairs):
        return lax.ppermute(array, "gz", pairs)

    def ends(array):
        return [lax.dynamic_slice_in_dim(array, start, HALO, 0) for start in (near_start, far_start)]

    my_labels, my_right = ends(labels), ends(right_side)
    near_labels = send(my_labels[0], across)
    near_right = send(my_right[0], across)
    far_labels = send(my_labels[1], inside)
    far_right = send(my_right[1], inside)

    tables, factors, *state, near, far = call(
        start_kernel,
        (my_labels[0], my_right[0], my_labels[1], my_right[1], far_labels, far_right, tensor_table, bounds),
        (tables, factors, field, cross_links, inplane_links, reaction, rest, field, plane, plane),
        0,
        LIMITS[0],
        10**8,
        halves,
        smem_count=2,
    )
    far_second = send(far, inside)
    near_second = send(near, across)

    *state, far, summed = call(
        middle_kernel,
        (*state, tables, factors, my_labels[0], far_second, near_labels),
        tuple(array(*s.shape) for s in state) + (plane, inner),
        6,
        LIMITS[1],
        10**8,
        halves,
    )
    far_third = send(far, inside)
    first, cross_links, inplane_links, reaction, rest, second = state
    links = (cross_links, inplane_links, reaction, factors)
    first, second, rest, solved = call(
        late_kernel,
        (first, second, rest, *links, near_right, summed),
        (field, field, array(*rest.shape), block),
        3,
        LIMITS[2],
        10**8,
        [pltpu.VMEM((HALO, rows, columns), jnp.float32), pltpu.SemaphoreType.DMA((depth,))],
        kept=3,
    )
    *_, residual, squares = call(
        last_kernel,
        (first, second, rest, *links, near_second, far_third),
        (field, field, array(*rest.shape), block, array(count, LANES)),
        3,
        LIMITS[3],
        10**8,
        [pltpu.SemaphoreType.DMA((depth, tiles))],
        kept=3,
    )
    gathered = lax.all_to_all(squares, "gz", 0, 0, tiled=True)
    return solved, residual, jnp.sqrt(jnp.sum(gathered[:, 0])).reshape(1)


def solution(mesh):
    whole = P(("groups", "gz"), None, None)
    return jax.shard_map(
        per_device,
        mesh=mesh,
        in_specs=(whole, P("groups", None), P("groups"), whole),
        out_specs=(whole, whole, P("groups")),
        check_vma=False,
    )
```

```python
import jax
import jax.numpy as jnp
from jax import lax
from jax.experimental import pallas as pl
from jax.experimental.pallas import tpu as pltpu
from jax.sharding import PartitionSpec as P


ITERS = 3
PHASES = 8
LANES = 128
SUB = 8
PAD = 8
BELOW = 8
RIM = 16
RIM_BELOW = 24
HALO = 2
OPERATOR_UNROLL = 16
LIMITS = (9, 9, 6, 6)

steps = (
    (1, 0, 0),
    (0, 1, 0),
    (0, 0, 1),
    (1, 1, 0),
    (1, -1, 0),
    (1, 0, 1),
    (1, 0, -1),
    (0, 1, 1),
    (0, 1, -1),
)
cross = [d for d, step in enumerate(steps) if step[0]]
inplane = [d for d, step in enumerate(steps) if not step[0]]


def slots(directions):
    order = [(d, 0) for d in directions] + [(d, 1) for d in directions if steps[d][2]]
    return {key: k for k, key in enumerate(order)}


cross_slots, inplane_slots = slots(cross), slots(inplane)


def splat(value):
    return jnp.full((SUB, LANES), value, jnp.float32)


def chebyshev(bounds_ref):
    lower, upper = splat(bounds_ref[0]), splat(bounds_ref[1])
    centre = (upper + lower) / 2.0
    half = (upper - lower) / 2.0
    sigma = centre / half
    rho = 1.0 / sigma
    factors = []
    for _ in range(ITERS):
        rho_new = 1.0 / (2.0 * sigma - rho)
        factors.append((rho_new * rho, 2.0 * rho_new / half))
        rho = rho_new
    return 1.0 / centre, factors


def each_block(rows, body, carry=0, unroll=None):
    count = rows // SUB
    unroll = min(unroll or 32, count)

    def step(k, carry):
        return body(pl.multiple_of(k * SUB, SUB), carry)

    carry = lax.fori_loop(0, count - count % unroll, step, carry, unroll=unroll)
    for k in range(count - count % unroll, count):
        carry = body(k * SUB, carry)
    return carry


def lane_shifted(values, dz, edge):
    lane = lax.broadcasted_iota(jnp.int32, (SUB, LANES), 1)
    turned = [pltpu.roll(value, LANES - 1 if dz == 1 else 1, 1) for value in values]
    if dz == 1:
        beyond = turned[1:] + [edge]
        return [jnp.where(lane == LANES - 1, b, t) for t, b in zip(turned, beyond)]
    beyond = [edge] + turned[:-1]
    return [jnp.where(lane == 0, b, t) for t, b in zip(turned, beyond)]


def put_field(field, plane, row, values):
    zero = splat(0.0)
    for variant, dz in ((0, 0), (1, 1), (2, -1)):
        shifted = lane_shifted(values, dz, zero) if dz else values
        for c, value in enumerate(shifted):
            field[plane, c, variant, pl.ds(row + PAD, SUB), :] = value


def field_rims(field, plane, tiles, rows):
    for variant in range(3):
        for c in range(tiles):
            field[plane, c, variant, pl.ds(0, PAD), :] = splat(0.0)
            field[plane, c, variant, pl.ds(rows + PAD, PAD), :] = splat(0.0)


def tile(ref, plane, c, row):
    return ref[plane, pl.ds(row, SUB), pl.ds(c * LANES, LANES)]


def put_tile(ref, plane, c, row, value):
    ref[plane, pl.ds(row, SUB), pl.ds(c * LANES, LANES)] = value


def put_tables(tables_ref, table_ref, flip):
    turn = jnp.where(splat(flip.astype(jnp.float32)) > 0.5, -0.5, 0.5)
    for phase in range(PHASES):
        k = [splat(table_ref[phase, column]) for column in range(7)]
        size = [jnp.abs(value) for value in k]
        values = (
            0.5 * (k[0] - size[3] - size[4]),
            turn * k[3],
            turn * k[4],
            0.5 * (k[1] - size[3] - size[5]),
            0.5 * (k[2] - size[4] - size[5]),
            0.5 * k[5],
            k[6],
        )
        for place, value in enumerate(values):
            tables_ref[phase, place] = value


def put_factors(factors_ref, bounds_ref):
    inverse, factors = chebyshev(bounds_ref)
    for k, value in enumerate([inverse] + [value for pair in factors for value in pair]):
        factors_ref[k] = value


def get_factors(factors_ref):
    pairs = [(factors_ref[1 + 2 * k], factors_ref[2 + 2 * k]) for k in range(ITERS)]
    return factors_ref[0], pairs


class Half:
    def __init__(self, tables_ref, refs, tiles, rows):
        self.refs, self.tiles, self.rows = refs, tiles, rows
        self.tables = [
            ([tables_ref[phase, k] for k in range(3)], [tables_ref[phase, k] for k in range(3, 7)])
            for phase in range(PHASES)
        ]
        for ref, slots_of in zip(refs, (cross_slots, inplane_slots)):
            for slot in range(ref.shape[0]):
                for k in range(len(slots_of)):
                    for c in range(tiles):
                        for start in (0, SUB, rows + RIM, rows + RIM + SUB):
                            ref[slot, c, k, pl.ds(start, SUB), :] = splat(0.0)

    def fill(self, slot, read, mask=None, reaction=None):
        for group in range(2 if reaction else 1):
            tables = [t[group] for t in self.tables]
            if mask is not None:
                tables = [[mask * value for value in t] for t in tables]
            ref, at = (self.refs[1], 0) if group else (self.refs[0], slot)
            places = inplane_slots if group else cross_slots

            def body(row, carry):
                found = {}
                for c in range(self.tiles):
                    label = read(c, row)
                    bits = [(label & (1 << b)) != 0 for b in range(3)]
                    looked = []
                    for column in range(len(tables[0])):
                        level = [t[column] for t in tables]
                        for bit in bits:
                            level = [jnp.where(bit, b, a) for a, b in zip(level[::2], level[1::2])]
                        looked.append(level[0])
                    if group == 0:
                        values = {0: looked[0]}
                        signed = zip((3, 5), looked[1:])
                    else:
                        values = {1: looked[0], 2: looked[1]}
                        signed = [(7, looked[2])]
                        reaction[0][reaction[1], c, pl.ds(row, SUB), :] = looked[3]
                    for d, value in signed:
                        values[d] = jnp.maximum(value, 0.0)
                        values[d + 1] = jnp.maximum(-value, 0.0)
                    for d, value in values.items():
                        ref[at, c, places[d, 0], pl.ds(row + RIM, SUB), :] = value
                        found.setdefault(d, []).append(value)
                for d, values in found.items():
                    if steps[d][2]:
                        for c, value in enumerate(lane_shifted(values, steps[d][2], splat(0.0))):
                            ref[at, c, places[d, 1], pl.ds(row + RIM, SUB), :] = value
                return carry

            each_block(self.rows, body)

    def link(self, slot, other, out, at):
        directions, places = (cross, cross_slots) if other is not None else (inplane, inplane_slots)
        ref = self.refs[0 if other is not None else 1]
        slot, other = (slot, other) if other is not None else (0, 0)

        def body(row, carry):
            for d in directions:
                _, dy, dz = steps[d]
                near = pl.ds(row + RIM - PAD, SUB)
                far = pl.ds(row + RIM - PAD + dy, SUB)
                ahead = [ref[other, c, places[d, 1 if dz else 0], far, :] for c in range(self.tiles)]
                values = [ref[slot, c, places[d, 0], near, :] + ahead[c] for c in range(self.tiles)]
                for c, value in enumerate(values):
                    out[at, c, places[d, 0], pl.ds(row, SUB), :] = value
                if dz:
                    edge = ref[other, 0 if dz == 1 else self.tiles - 1, places[d, 0], far, :]
                    for c, value in enumerate(lane_shifted(values, -dz, edge)):
                        out[at, c, places[d, 1], pl.ds(row, SUB), :] = value
            return carry

        each_block(self.rows + 2 * PAD, body, unroll=17)


def run_operator(field, links, planes, device, use, parts={}, carry=0):
    cross_ref, inplane_ref, reaction_ref = links

    def body(row, carry):
        held = {}

        def value(q, c, dy, dz):
            key = (q, c, dy, dz)
            if key not in held:
                held[key] = field[q + HALO, c, dz % 3, pl.ds(row + PAD + dy, SUB), :]
            return held[key]

        def image(q, c):
            here = value(q, c, 0, 0)
            wanted = parts.get(q, (-1, 0, 1))
            sums = [reaction_ref[q + 1, c, pl.ds(row, SUB), :] * here] if 0 in wanted else []
            for d, (dx, dy, dz) in enumerate(steps):
                places = cross_slots if dx else inplane_slots
                ref, base = (cross_ref, HALO) if dx else (inplane_ref, 1)
                for sign in (1, -1):
                    if sign * dx not in wanted:
                        continue
                    if sign == 1:
                        link = ref[q + base, c, places[d, 0], pl.ds(row + PAD, SUB), :]
                    else:
                        key = places[d, 1 if dz else 0]
                        link = ref[q + base - dx, c, key, pl.ds(row + PAD - dy, SUB), :]
                    term = link * (here - value(q + sign * dx, c, sign * dy, sign * dz))
                    sums = sums[1:] + [sums[0] + term] if len(sums) == 3 else sums + [term]
            return sums[0] + (sums[1] + sums[2])

        for q in planes:
            images = [image(q, c) for c in range(device.tiles)]
            carry = use(q, row, images, [value(q, c, 0, 0) for c in range(device.tiles)], carry)
        return carry

    return each_block(device.rows, body, carry, unroll=OPERATOR_UNROLL)


class Device:
    def __init__(self, shape):
        self.depth, self.rows, self.tiles = shape[0], shape[1], shape[2] // LANES
        self.place, self.count = lax.axis_index("gz"), lax.axis_size("gz")
        self.flip = self.place % 2
        joined = jnp.logical_and(self.place > 0, self.place < self.count - 1)
        self.joined = splat(joined.astype(jnp.float32))

    def own(self, q):
        return jnp.where(self.flip == 1, self.depth - 1 - q, q)

    def sent(self, q):
        return jnp.where(self.flip == 1, 1 - q % HALO, q % HALO)

    def halo(self, q):
        far = q >= self.depth
        first = (q == self.depth) if far else (q == -1)
        turned = self.flip == (1 if far else 0)
        return jnp.where(turned, 1, 0) if first else jnp.where(turned, 0, 1)


class Solve:
    def __init__(self, device, refs, factors, right=None):
        self.device, self.factors, self.right = device, factors, right
        self.first, self.second, *self.links, self.rest = refs

    def advance(self, iteration, planes, direct=(), parts={}, copies={}, keep=None):
        device, rest_ref = self.device, self.rest
        old, new = (self.first, self.second) if iteration == 0 else (self.second, self.first)
        ahead, behind = self.factors[iteration]
        if iteration == 2:
            old, new = new, old
        for q in direct:
            if q < 0:
                field_rims(new, q + HALO, device.tiles, device.rows)

        def use(q, row, images, here, carry):
            block = pl.ds(row, SUB)
            if self.right and iteration == 0 and q < 0:
                before = [self.right(q, c, row) for c in range(device.tiles)]
            else:
                before = [rest_ref[q + 1, c, block, :] for c in range(device.tiles)]
            rest = [b - image for b, image in zip(before, images)]
            if q < 0:
                rest = [device.joined * r for r in rest]
            for c, r in enumerate(rest):
                rest_ref[q + 1, c, block, :] = r
            if q in direct:
                values = [ahead * h + behind * r for h, r in zip(here, rest)]
                if q in copies:
                    for c, v in enumerate(values):
                        put_tile(copies[q], 0, c, row, v)
                if keep and 0 <= q:
                    for c, (h, v) in enumerate(zip(here, values)):
                        keep(q, c, row, new[q + HALO, c, 0, pl.ds(row + PAD, SUB), :] + h + v)
                put_field(new, q + HALO, row, values)
            return carry

        run_operator(old, self.links, planes, device, use, parts)

    def receive(self, field, q, read):
        field_rims(field, q + HALO, self.device.tiles, self.device.rows)

        def body(row, carry):
            put_field(field, q + HALO, row, [read(c, row) for c in range(self.device.tiles)])
            return carry

        each_block(self.device.rows, body)


def start_kernel(*refs):
    near_labels_ref, near_right_ref, far_labels_ref, far_right_ref, beside_labels_ref, beside_right_ref = refs[:6]
    table_ref, bounds_ref, tables_ref, factors_ref = refs[6:10]
    first_ref, cross_ref, inplane_ref, reaction_ref, rest_ref, second_ref, near_ref, far_ref = refs[10:18]
    halves = refs[18:]
    device = Device((2 * HALO,) + near_labels_ref.shape[1:])
    depth, rows, tiles = device.depth, device.rows, device.tiles
    put_factors(factors_ref, bounds_ref)
    inverse, factors = get_factors(factors_ref)
    put_tables(tables_ref, table_ref, device.flip)
    half = Half(tables_ref, halves, tiles, rows)

    def read(q, near, far, beside):
        if q == depth:
            ref, index = beside, device.halo(q)
        else:
            ref, index = near if q < HALO else far, device.sent(q)
        return lambda c, row: tile(ref, index, c, row)

    for q in range(depth + 1):
        field_rims(first_ref, q + HALO, tiles, rows)
        field_rims(second_ref, q + HALO, tiles, rows)
        right = read(q, near_right_ref, far_right_ref, beside_right_ref)

        def body(row, carry):
            values = [right(c, row) for c in range(tiles)]
            if q < depth:
                for c, value in enumerate(values):
                    rest_ref[q + 1, c, pl.ds(row, SUB), :] = value
            put_field(first_ref, q + HALO, row, [value * inverse for value in values])
            return carry

        each_block(rows, body)
        labels = read(q, near_labels_ref, far_labels_ref, beside_labels_ref)
        half.fill(q % 2, labels, None, (reaction_ref, q + 1) if q < depth else None)
        if q:
            half.link((q - 1) % 2, q % 2, cross_ref, q - 1 + HALO)
        if q < depth:
            half.link(q % 2, None, inplane_ref, q + 1)

    solve = Solve(device, (first_ref, second_ref, cross_ref, inplane_ref, reaction_ref, rest_ref), factors)
    solve.advance(0, range(depth), range(1, depth), parts={0: (0, 1)}, copies={1: near_ref, depth - 1: far_ref})


def middle_kernel(*refs):
    tables_ref, factors_ref, sent_labels_ref, far_second_ref, near_labels_ref = refs[6:11]
    first_ref, cross_ref, inplane_ref, reaction_ref, rest_ref, second_ref, far_ref, sum_ref, *halves = refs[11:]
    device = Device((2 * HALO,) + near_labels_ref.shape[1:])
    depth = device.depth
    _, factors = get_factors(factors_ref)
    solve = Solve(device, (first_ref, second_ref, cross_ref, inplane_ref, reaction_ref, rest_ref), factors)
    solve.receive(second_ref, depth, lambda c, row: tile(far_second_ref, 0, c, row))

    def keep(q, c, row, value):
        put_tile(sum_ref, q - HALO, c, row, value)

    solve.advance(
        1,
        range(1, depth),
        range(HALO, depth),
        parts={1: (0, 1)},
        copies={depth - 1: far_ref},
        keep=keep,
    )
    solve.advance(2, range(HALO, depth), parts={HALO: (0, 1), depth - 1: (-1, 0)})

    def labels(ref, index):
        return lambda c, row: tile(ref, index, c, row)

    half = Half(tables_ref, halves, device.tiles, device.rows)
    half.fill(0, labels(sent_labels_ref, device.sent(0)))
    half.fill(1, labels(near_labels_ref, device.halo(-1)), device.joined, (reaction_ref, 0))
    half.link(1, None, inplane_ref, 0)
    half.link(1, 0, cross_ref, HALO - 1)
    half.fill(0, labels(near_labels_ref, device.halo(-2)), device.joined)
    half.link(0, 1, cross_ref, HALO - 2)


def late_kernel(*refs):
    *links, factors_ref, near_right_ref, sum_ref = refs[3:9]
    first_ref, second_ref, rest_ref, solution_ref, ready_ref, sems = refs[9:]
    device = Device(solution_ref.shape)
    depth = device.depth
    inverse, factors = get_factors(factors_ref)
    copies = [
        pltpu.make_async_copy(
            ready_ref.at[q] if q < HALO else sum_ref.at[q - HALO], solution_ref.at[device.own(q)], sems.at[q]
        )
        for q in range(depth)
    ]
    for copy in copies[HALO:]:
        copy.start()

    def right(q, c, row):
        return tile(near_right_ref, device.halo(q), c, row)

    def keep(q, c, row, value):
        put_tile(ready_ref, q, c, row, value)

    solve = Solve(device, (first_ref, second_ref, *links, rest_ref), factors, right)
    for q in (-1, -2):
        index = device.halo(q)
        solve.receive(first_ref, q, lambda c, row: tile(near_right_ref, index, c, row) * inverse)
    solve.advance(0, [-1, 0], [-1, 0], parts={0: (-1,)})
    solve.advance(1, [-1, 0, 1], [0, 1], parts={-1: (0, 1), 1: (-1,)}, keep=keep)
    for copy in copies[:HALO]:
        copy.start()
    solve.advance(2, range(HALO + 1), parts={0: (0, 1), HALO: (-1,)})
    for copy in copies:
        copy.wait()


def last_kernel(*refs):
    *links, factors_ref, near_second_ref, far_third_ref = refs[3:9]
    first_ref, second_ref, rest_ref, residual_ref, squares_ref, sems = refs[9:]
    device = Device(residual_ref.shape)
    depth = device.depth
    copies = {
        q: [
            pltpu.make_async_copy(
                rest_ref.at[q + 1, c],
                residual_ref.at[device.own(q), :, pl.ds(c * LANES, LANES)],
                sems.at[q, c],
            )
            for c in range(device.tiles)
        ]
        for q in range(depth)
    }
    for q in range(1, depth - 1):
        for copy in copies[q]:
            copy.start()
    _, factors = get_factors(factors_ref)
    solve = Solve(device, (first_ref, second_ref, *links, rest_ref), factors)
    solve.receive(first_ref, depth, lambda c, row: tile(far_third_ref, 0, c, row))
    solve.receive(second_ref, -2, lambda c, row: tile(near_second_ref, 0, c, row))
    solve.advance(1, [-1], [-1], parts={-1: (-1,)})

    def use(q, row, images, here, carry):
        for c, image in enumerate(images):
            for plane in range(depth - 1) if q == 0 else [q]:
                rest = rest_ref[plane + 1, c, pl.ds(row, SUB), :]
                if plane == q:
                    rest = rest - image
                    rest_ref[plane + 1, c, pl.ds(row, SUB), :] = rest
                carry = carry + rest * rest
        return carry

    ends = {0: (-1,), depth - 1: (1,)}
    total = run_operator(first_ref, links, list(ends), device, use, ends, splat(0.0))
    for q in ends:
        for copy in copies[q]:
            copy.start()
    squares_ref[...] = jnp.broadcast_to(jnp.sum(total), squares_ref.shape)
    for q in range(depth):
        for copy in copies[q]:
            copy.wait()


def per_device(labels, tensor_table, bounds, right_side):
    depth, rows, columns = labels.shape
    if depth != 2 * HALO or columns % LANES or rows % SUB:
        raise ValueError("unsupported block")
    tiles = columns // LANES
    count = lax.axis_size("gz")
    odd = lax.axis_index("gz") % 2

    vmem = pl.BlockSpec(memory_space=pltpu.VMEM)
    smem = pl.BlockSpec(memory_space=pltpu.SMEM)
    hbm = pl.BlockSpec(memory_space=pltpu.HBM)

    def array(*shape):
        return jax.ShapeDtypeStruct(shape, jnp.float32)

    below = rows + PAD + BELOW
    field = array(depth + HALO + 1, tiles, 3, below, LANES)
    cross_links = array(depth + HALO, tiles, len(cross_slots), below, LANES)
    inplane_links = array(depth + 1, tiles, len(inplane_slots), below, LANES)
    reaction = rest = array(depth + 1, tiles, rows, LANES)
    inner = array(depth - HALO, rows, columns)
    plane = array(1, rows, columns)
    block = array(depth, rows, columns)
    tables, factors = array(PHASES, 7, SUB, LANES), array(1 + 2 * ITERS, SUB, LANES)
    halves = [
        pltpu.VMEM((planes, tiles, len(places), rows + RIM + RIM_BELOW, LANES), jnp.float32)
        for planes, places in ((2, cross_slots), (1, inplane_slots))
    ]

    def call(kernel, arguments, out_shape, aliased, limit, flops, scratch=(), smem_count=0, kept=None):
        return pl.pallas_call(
            kernel,
            out_shape=out_shape,
            in_specs=[vmem] * (len(arguments) - smem_count) + [smem] * smem_count,
            out_specs=[hbm if k == kept else vmem for k in range(len(out_shape))],
            scratch_shapes=list(scratch),
            input_output_aliases={k: k for k in range(aliased)},
            compiler_params=pltpu.CompilerParams(vmem_limit_bytes=limit << 20),
            cost_estimate=pl.CostEstimate(flops=flops, bytes_accessed=1 << 20, transcendentals=0),
        )(*arguments)

    inside = [(i, i ^ 1) for i in range(count)]
    across = [(i, i + 1) for i in range(1, count - 1, 2)]
    across += [(j, i) for i, j in across]
    near_start = odd * (depth - HALO)
    far_start = (1 - odd) * (depth - HALO)

    def send(array, pairs):
        return lax.ppermute(array, "gz", pairs)

    def ends(array):
        return [lax.dynamic_slice_in_dim(array, start, HALO, 0) for start in (near_start, far_start)]

    my_labels, my_right = ends(labels), ends(right_side)
    near_labels = send(my_labels[0], across)
    near_right = send(my_right[0], across)
    far_labels = send(my_labels[1], inside)
    far_right = send(my_right[1], inside)

    tables, factors, *state, near, far = call(
        start_kernel,
        (my_labels[0], my_right[0], my_labels[1], my_right[1], far_labels, far_right, tensor_table, bounds),
        (tables, factors, field, cross_links, inplane_links, reaction, rest, field, plane, plane),
        0,
        LIMITS[0],
        10**8,
        halves,
        smem_count=2,
    )
    far_second = send(far, inside)
    near_second = send(near, across)

    *state, far, summed = call(
        middle_kernel,
        (*state, tables, factors, my_labels[0], far_second, near_labels),
        tuple(array(*s.shape) for s in state) + (plane, inner),
        6,
        LIMITS[1],
        10**8,
        halves,
    )
    far_third = send(far, inside)
    first, cross_links, inplane_links, reaction, rest, second = state
    links = (cross_links, inplane_links, reaction, factors)
    first, second, rest, solved = call(
        late_kernel,
        (first, second, rest, *links, near_right, summed),
        (field, field, array(*rest.shape), block),
        3,
        LIMITS[2],
        10**8,
        [pltpu.VMEM((HALO, rows, columns), jnp.float32), pltpu.SemaphoreType.DMA((depth,))],
        kept=3,
    )
    *_, residual, squares = call(
        last_kernel,
        (first, second, rest, *links, near_second, far_third),
        (field, field, array(*rest.shape), block, array(count, LANES)),
        3,
        LIMITS[3],
        10**8,
        [pltpu.SemaphoreType.DMA((depth, tiles))],
        kept=3,
    )
    gathered = lax.all_to_all(squares, "gz", 0, 0, tiled=True)
    return solved, residual, jnp.sqrt(jnp.sum(gathered[:, 0])).reshape(1)


def solution(mesh):
    whole = P(("groups", "gz"), None, None)
    return jax.shard_map(
        per_device,
        mesh=mesh,
        in_specs=(whole, P("groups", None), P("groups"), whole),
        out_specs=(whole, whole, P("groups")),
        check_vma=False,
    )
```

```python
import jax
import jax.numpy as jnp
from jax import lax
from jax.experimental import pallas as pl
from jax.experimental.pallas import tpu as pltpu
from jax.sharding import PartitionSpec as P


ITERS = 3
PHASES = 8
LANES = 128
SUB = 8
PAD = 8
BELOW = 8
RIM = 16
RIM_BELOW = 24
HALO = 2
OPERATOR_UNROLL = 16
LIMITS = (9, 5, 5, 5)

steps = (
    (1, 0, 0),
    (0, 1, 0),
    (0, 0, 1),
    (1, 1, 0),
    (1, -1, 0),
    (1, 0, 1),
    (1, 0, -1),
    (0, 1, 1),
    (0, 1, -1),
)
cross = [d for d, step in enumerate(steps) if step[0]]
inplane = [d for d, step in enumerate(steps) if not step[0]]


def slots(directions):
    order = [(d, 0) for d in directions] + [(d, 1) for d in directions if steps[d][2]]
    return {key: k for k, key in enumerate(order)}


cross_slots, inplane_slots = slots(cross), slots(inplane)


def splat(value):
    return jnp.full((SUB, LANES), value, jnp.float32)


def chebyshev(bounds_ref):
    lower, upper = splat(bounds_ref[0]), splat(bounds_ref[1])
    centre = (upper + lower) / 2.0
    half = (upper - lower) / 2.0
    sigma = centre / half
    rho = 1.0 / sigma
    factors = []
    for _ in range(ITERS):
        rho_new = 1.0 / (2.0 * sigma - rho)
        factors.append((rho_new * rho, 2.0 * rho_new / half))
        rho = rho_new
    return 1.0 / centre, factors


def each_block(rows, body, carry=0, unroll=None):
    count = rows // SUB
    unroll = min(unroll or 32, count)

    def step(k, carry):
        return body(pl.multiple_of(k * SUB, SUB), carry)

    carry = lax.fori_loop(0, count - count % unroll, step, carry, unroll=unroll)
    for k in range(count - count % unroll, count):
        carry = body(k * SUB, carry)
    return carry


def lane_shifted(values, dz, edge):
    lane = lax.broadcasted_iota(jnp.int32, (SUB, LANES), 1)
    turned = [pltpu.roll(value, LANES - 1 if dz == 1 else 1, 1) for value in values]
    if dz == 1:
        beyond = turned[1:] + [edge]
        return [jnp.where(lane == LANES - 1, b, t) for t, b in zip(turned, beyond)]
    beyond = [edge] + turned[:-1]
    return [jnp.where(lane == 0, b, t) for t, b in zip(turned, beyond)]


def put_field(field, plane, row, values):
    zero = splat(0.0)
    for variant, dz in ((0, 0), (1, 1), (2, -1)):
        shifted = lane_shifted(values, dz, zero) if dz else values
        for c, value in enumerate(shifted):
            field[plane, c, variant, pl.ds(row + PAD, SUB), :] = value


def field_rims(field, plane, tiles, rows):
    for variant in range(3):
        for c in range(tiles):
            field[plane, c, variant, pl.ds(0, PAD), :] = splat(0.0)
            field[plane, c, variant, pl.ds(rows + PAD, PAD), :] = splat(0.0)


def tile(ref, plane, c, row):
    return ref[plane, pl.ds(row, SUB), pl.ds(c * LANES, LANES)]


def label_of(ref):
    return lambda c, row: tile(ref, 0, c, row).astype(jnp.int32)


def put_tile(ref, plane, c, row, value):
    ref[plane, pl.ds(row, SUB), pl.ds(c * LANES, LANES)] = value


def put_tables(tables_ref, table_ref, flip):
    turn = jnp.where(splat(flip.astype(jnp.float32)) > 0.5, -0.5, 0.5)
    for phase in range(PHASES):
        k = [splat(table_ref[phase, column]) for column in range(7)]
        size = [jnp.abs(value) for value in k]
        values = (
            0.5 * (k[0] - size[3] - size[4]),
            turn * k[3],
            turn * k[4],
            0.5 * (k[1] - size[3] - size[5]),
            0.5 * (k[2] - size[4] - size[5]),
            0.5 * k[5],
            k[6],
        )
        for place, value in enumerate(values):
            tables_ref[phase, place] = value


def put_factors(factors_ref, bounds_ref):
    inverse, factors = chebyshev(bounds_ref)
    for k, value in enumerate([inverse] + [value for pair in factors for value in pair]):
        factors_ref[k] = value


def get_factors(factors_ref):
    pairs = [(factors_ref[1 + 2 * k], factors_ref[2 + 2 * k]) for k in range(ITERS)]
    return factors_ref[0], pairs


class Half:
    def __init__(self, tables_ref, refs, tiles, rows, clean=True):
        self.refs, self.tiles, self.rows = refs, tiles, rows
        self.tables = [
            ([tables_ref[phase, k] for k in range(3)], [tables_ref[phase, k] for k in range(3, 7)])
            for phase in range(PHASES)
        ]
        for ref, slots_of in zip(refs, (cross_slots, inplane_slots)):
            for slot in range(ref.shape[0] if clean else 0):
                for k in range(len(slots_of)):
                    for c in range(tiles):
                        for start in (0, SUB, rows + RIM, rows + RIM + SUB):
                            ref[slot, c, k, pl.ds(start, SUB), :] = splat(0.0)

    def fill(self, slot, read, mask=None, reaction=None):
        for group in range(2 if reaction else 1):
            tables = [t[group] for t in self.tables]
            if mask is not None:
                tables = [[mask * value for value in t] for t in tables]
            ref, at = (self.refs[1], 0) if group else (self.refs[0], slot)
            places = inplane_slots if group else cross_slots

            def body(row, carry):
                found = {}
                for c in range(self.tiles):
                    label = read(c, row)
                    bits = [(label & (1 << b)) != 0 for b in range(3)]
                    looked = []
                    for column in range(len(tables[0])):
                        level = [t[column] for t in tables]
                        for bit in bits:
                            level = [jnp.where(bit, b, a) for a, b in zip(level[::2], level[1::2])]
                        looked.append(level[0])
                    if group == 0:
                        values = {0: looked[0]}
                        signed = zip((3, 5), looked[1:])
                    else:
                        values = {1: looked[0], 2: looked[1]}
                        signed = [(7, looked[2])]
                        reaction[0][reaction[1], c, pl.ds(row, SUB), :] = looked[3]
                    for d, value in signed:
                        values[d] = jnp.maximum(value, 0.0)
                        values[d + 1] = jnp.maximum(-value, 0.0)
                    for d, value in values.items():
                        ref[at, c, places[d, 0], pl.ds(row + RIM, SUB), :] = value
                        found.setdefault(d, []).append(value)
                for d, values in found.items():
                    if steps[d][2]:
                        for c, value in enumerate(lane_shifted(values, steps[d][2], splat(0.0))):
                            ref[at, c, places[d, 1], pl.ds(row + RIM, SUB), :] = value
                return carry

            each_block(self.rows, body)

    def link(self, slot, other, out, at):
        directions, places = (cross, cross_slots) if other is not None else (inplane, inplane_slots)
        ref = self.refs[0 if other is not None else 1]
        slot, other = (slot, other) if other is not None else (0, 0)

        def body(row, carry):
            for d in directions:
                _, dy, dz = steps[d]
                near = pl.ds(row + RIM - PAD, SUB)
                far = pl.ds(row + RIM - PAD + dy, SUB)
                ahead = [ref[other, c, places[d, 1 if dz else 0], far, :] for c in range(self.tiles)]
                values = [ref[slot, c, places[d, 0], near, :] + ahead[c] for c in range(self.tiles)]
                for c, value in enumerate(values):
                    out[at, c, places[d, 0], pl.ds(row, SUB), :] = value
                if dz:
                    edge = ref[other, 0 if dz == 1 else self.tiles - 1, places[d, 0], far, :]
                    for c, value in enumerate(lane_shifted(values, -dz, edge)):
                        out[at, c, places[d, 1], pl.ds(row, SUB), :] = value
            return carry

        each_block(self.rows + 2 * PAD, body, unroll=17)


def run_operator(field, links, planes, device, use, parts={}, carry=0):
    cross_ref, inplane_ref, reaction_ref = links

    def body(row, carry):
        held = {}

        def value(q, c, dy, dz):
            key = (q, c, dy, dz)
            if key not in held:
                held[key] = field[q + HALO, c, dz % 3, pl.ds(row + PAD + dy, SUB), :]
            return held[key]

        def image(q, c):
            here = value(q, c, 0, 0)
            wanted = parts.get(q, (-1, 0, 1))
            sums = [reaction_ref[q + 1, c, pl.ds(row, SUB), :] * here] if 0 in wanted else []
            for d, (dx, dy, dz) in enumerate(steps):
                places = cross_slots if dx else inplane_slots
                ref, base = (cross_ref, HALO) if dx else (inplane_ref, 1)
                for sign in (1, -1):
                    if sign * dx not in wanted:
                        continue
                    if sign == 1:
                        link = ref[q + base, c, places[d, 0], pl.ds(row + PAD, SUB), :]
                    else:
                        key = places[d, 1 if dz else 0]
                        link = ref[q + base - dx, c, key, pl.ds(row + PAD - dy, SUB), :]
                    term = link * (here - value(q + sign * dx, c, sign * dy, sign * dz))
                    sums = sums[1:] + [sums[0] + term] if len(sums) == 3 else sums + [term]
            return sums[0] + (sums[1] + sums[2])

        for q in planes:
            images = [image(q, c) for c in range(device.tiles)]
            carry = use(q, row, images, [value(q, c, 0, 0) for c in range(device.tiles)], carry)
        return carry

    return each_block(device.rows, body, carry, unroll=OPERATOR_UNROLL)


class Device:
    def __init__(self, shape):
        self.depth, self.rows, self.tiles = shape[0], shape[1], shape[2] // LANES
        self.place, self.count = lax.axis_index("gz"), lax.axis_size("gz")
        self.flip = self.place % 2
        joined = jnp.logical_and(self.place > 0, self.place < self.count - 1)
        self.joined = splat(joined.astype(jnp.float32))

    def own(self, q):
        return jnp.where(self.flip == 1, self.depth - 1 - q, q)


class Solve:
    def __init__(self, device, refs, factors, right=None):
        self.device, self.factors, self.right = device, factors, right
        self.first, self.second, *self.links, self.rest = refs

    def advance(self, iteration, planes, direct=(), parts={}, copies={}, keep=None):
        device, rest_ref = self.device, self.rest
        old, new = (self.first, self.second) if iteration == 0 else (self.second, self.first)
        ahead, behind = self.factors[iteration]
        if iteration == 2:
            old, new = new, old
        for q in direct:
            if q < 0:
                field_rims(new, q + HALO, device.tiles, device.rows)

        def use(q, row, images, here, carry):
            block = pl.ds(row, SUB)
            if self.right and iteration == 0 and q < 0:
                before = [self.right(q, c, row) for c in range(device.tiles)]
            else:
                before = [rest_ref[q + 1, c, block, :] for c in range(device.tiles)]
            rest = [b - image for b, image in zip(before, images)]
            if q < 0:
                rest = [device.joined * r for r in rest]
            for c, r in enumerate(rest):
                rest_ref[q + 1, c, block, :] = r
            if q in direct:
                values = [ahead * h + behind * r for h, r in zip(here, rest)]
                if q in copies:
                    for c, v in enumerate(values):
                        put_tile(copies[q], 0, c, row, v)
                if keep and 0 <= q:
                    for c, (h, v) in enumerate(zip(here, values)):
                        keep(q, c, row, new[q + HALO, c, 0, pl.ds(row + PAD, SUB), :] + h + v)
                put_field(new, q + HALO, row, values)
            return carry

        run_operator(old, self.links, planes, device, use, parts)

    def receive(self, field, q, read):
        field_rims(field, q + HALO, self.device.tiles, self.device.rows)

        def body(row, carry):
            put_field(field, q + HALO, row, [read(c, row) for c in range(self.device.tiles)])
            return carry

        each_block(self.device.rows, body)


def start_kernel(*refs):
    *pairs, table_ref, bounds_ref, tables_ref, factors_ref = refs[:9]
    first_ref, cross_ref, inplane_ref, reaction_ref, rest_ref, second_ref, near_ref, far_ref = refs[9:17]
    halves = refs[17:]
    device = Device((len(pairs) - 1,) + pairs[0].shape[1:])
    depth, rows, tiles = device.depth, device.rows, device.tiles
    put_factors(factors_ref, bounds_ref)
    inverse, factors = get_factors(factors_ref)
    put_tables(tables_ref, table_ref, device.flip)
    half = Half(tables_ref, halves, tiles, rows)

    for q, pair_ref in enumerate(pairs):
        field_rims(first_ref, q + HALO, tiles, rows)
        field_rims(second_ref, q + HALO, tiles, rows)

        def body(row, carry):
            values = [tile(pair_ref, 1, c, row) for c in range(tiles)]
            if q < depth:
                for c, value in enumerate(values):
                    rest_ref[q + 1, c, pl.ds(row, SUB), :] = value
            put_field(first_ref, q + HALO, row, [value * inverse for value in values])
            return carry

        each_block(rows, body)
        half.fill(q % 2, label_of(pair_ref), None, (reaction_ref, q + 1) if q < depth else None)
        if q:
            half.link((q - 1) % 2, q % 2, cross_ref, q - 1 + HALO)
        if q < depth:
            half.link(q % 2, None, inplane_ref, q + 1)

    solve = Solve(device, (first_ref, second_ref, cross_ref, inplane_ref, reaction_ref, rest_ref), factors)
    solve.advance(0, range(depth), range(1, depth), parts={0: (0, 1)}, copies={1: near_ref, depth - 1: far_ref})


def middle_kernel(*refs):
    tables_ref, factors_ref, own_ref, far_second_ref, near_ref = refs[6:11]
    first_ref, cross_ref, inplane_ref, reaction_ref, rest_ref, second_ref, far_ref, sum_ref, *halves = refs[11:]
    depth = rest_ref.shape[0] - 1
    device = Device((depth,) + near_ref.shape[1:])
    inverse, factors = get_factors(factors_ref)
    half = Half(tables_ref, halves, device.tiles, device.rows)
    half.fill(0, label_of(own_ref))
    half.fill(1, label_of(near_ref), device.joined, (reaction_ref, 0))
    half.link(1, None, inplane_ref, 0)
    half.link(1, 0, cross_ref, HALO - 1)

    def right(q, c, row):
        return tile(near_ref, 1, c, row)

    def keep(q, c, row, value):
        put_tile(sum_ref, q - 1, c, row, value)

    solve = Solve(device, (first_ref, second_ref, cross_ref, inplane_ref, reaction_ref, rest_ref), factors, right)
    solve.receive(first_ref, -1, lambda c, row: tile(near_ref, 1, c, row) * inverse)
    solve.advance(0, [-1, 0], [0], parts={-1: (0, 1), 0: (-1,)})
    solve.receive(second_ref, depth, lambda c, row: tile(far_second_ref, 0, c, row))
    solve.advance(1, range(depth), range(1, depth), parts={0: (0, 1)}, copies={depth - 1: far_ref}, keep=keep)
    solve.advance(2, range(1, depth), parts={1: (0, 1), depth - 1: (-1, 0)})


def late_kernel(*refs):
    inplane_ref, reaction_ref, factors_ref, tables_ref, near_ref, sum_ref = refs[5:11]
    first_ref, second_ref, rest_ref, cross_ref, half_ref, solution_ref, ready_ref, sems = refs[11:]
    device = Device(solution_ref.shape)
    depth = device.depth
    inverse, factors = get_factors(factors_ref)
    copies = [
        pltpu.make_async_copy(
            sum_ref.at[q - 1] if q else ready_ref.at[0], solution_ref.at[device.own(q)], sems.at[q]
        )
        for q in range(depth)
    ]
    for copy in copies[1:]:
        copy.start()
    half = Half(tables_ref, (half_ref,), device.tiles, device.rows, clean=False)
    half.fill(0, label_of(near_ref), device.joined)
    half.link(0, 1, cross_ref, HALO - 2)

    def keep(q, c, row, value):
        put_tile(ready_ref, q, c, row, value)

    solve = Solve(device, (first_ref, second_ref, cross_ref, inplane_ref, reaction_ref, rest_ref), factors)
    solve.receive(first_ref, -2, lambda c, row: tile(near_ref, 1, c, row) * inverse)
    solve.advance(0, [-1], [-1], parts={-1: (-1,)})
    solve.advance(1, [-1, 0], [0], parts={-1: (0, 1), 0: (-1,)}, keep=keep)
    copies[0].start()
    solve.advance(2, [0, 1], parts={0: (0, 1), 1: (-1,)})
    for copy in copies:
        copy.wait()


def last_kernel(*refs):
    *links, factors_ref, near_second_ref, far_third_ref = refs[3:9]
    first_ref, second_ref, rest_ref, residual_ref, squares_ref, sems = refs[9:]
    device = Device(residual_ref.shape)
    depth = device.depth
    copies = {
        q: [
            pltpu.make_async_copy(
                rest_ref.at[q + 1, c],
                residual_ref.at[device.own(q), :, pl.ds(c * LANES, LANES)],
                sems.at[q, c],
            )
            for c in range(device.tiles)
        ]
        for q in range(depth)
    }
    for q in range(1, depth - 1):
        for copy in copies[q]:
            copy.start()
    _, factors = get_factors(factors_ref)
    solve = Solve(device, (first_ref, second_ref, *links, rest_ref), factors)
    solve.receive(first_ref, depth, lambda c, row: tile(far_third_ref, 0, c, row))
    solve.receive(second_ref, -2, lambda c, row: tile(near_second_ref, 0, c, row))
    solve.advance(1, [-1], [-1], parts={-1: (-1,)})

    def use(q, row, images, here, carry):
        for c, image in enumerate(images):
            for plane in range(depth - 1) if q == 0 else [q]:
                rest = rest_ref[plane + 1, c, pl.ds(row, SUB), :]
                if plane == q:
                    rest = rest - image
                    rest_ref[plane + 1, c, pl.ds(row, SUB), :] = rest
                carry = carry + rest * rest
        return carry

    ends = {0: (-1,), depth - 1: (1,)}
    total = run_operator(first_ref, links, list(ends), device, use, ends, splat(0.0))
    for q in ends:
        for copy in copies[q]:
            copy.start()
    squares_ref[...] = jnp.broadcast_to(jnp.sum(total), squares_ref.shape)
    for q in range(depth):
        for copy in copies[q]:
            copy.wait()


def per_device(labels, tensor_table, bounds, right_side):
    depth, rows, columns = labels.shape
    if depth != 2 * HALO or columns % LANES or rows % SUB:
        raise ValueError("unsupported block")
    tiles = columns // LANES
    count = lax.axis_size("gz")
    odd = lax.axis_index("gz") % 2

    vmem = pl.BlockSpec(memory_space=pltpu.VMEM)
    smem = pl.BlockSpec(memory_space=pltpu.SMEM)
    hbm = pl.BlockSpec(memory_space=pltpu.HBM)

    def array(*shape):
        return jax.ShapeDtypeStruct(shape, jnp.float32)

    below = rows + PAD + BELOW
    field = array(depth + HALO + 1, tiles, 3, below, LANES)
    cross_links = array(depth + HALO, tiles, len(cross_slots), below, LANES)
    inplane_links = array(depth + 1, tiles, len(inplane_slots), below, LANES)
    reaction = rest = array(depth + 1, tiles, rows, LANES)
    inner = array(depth - 1, rows, columns)
    plane = array(1, rows, columns)
    block = array(depth, rows, columns)
    tables, factors = array(PHASES, 7, SUB, LANES), array(1 + 2 * ITERS, SUB, LANES)
    halves = [
        pltpu.VMEM((planes, tiles, len(places), rows + RIM + RIM_BELOW, LANES), jnp.float32)
        for planes, places in ((2, cross_slots), (1, inplane_slots))
    ]

    def call(kernel, arguments, out_shape, aliased, limit, flops, scratch=(), smem_count=0, kept=None):
        return pl.pallas_call(
            kernel,
            out_shape=out_shape,
            in_specs=[vmem] * (len(arguments) - smem_count) + [smem] * smem_count,
            out_specs=[hbm if k == kept else vmem for k in range(len(out_shape))],
            scratch_shapes=list(scratch),
            input_output_aliases={k: k for k in range(aliased)},
            compiler_params=pltpu.CompilerParams(vmem_limit_bytes=limit << 20),
            cost_estimate=pl.CostEstimate(flops=flops, bytes_accessed=1 << 20, transcendentals=0),
        )(*arguments)

    inside = [(i, i ^ 1) for i in range(count)]
    across = [(i, i + 1) for i in range(1, count - 1, 2)]
    across += [(j, i) for i, j in across]

    def send(array, pairs):
        return lax.ppermute(array, "gz", pairs)

    def pair(q, labels, right_side):
        index = jnp.where(odd == 1, depth - 1 - q, q)
        own_labels = lax.dynamic_slice_in_dim(labels, index, 1, 0).astype(jnp.float32)
        return jnp.concatenate([own_labels, lax.dynamic_slice_in_dim(right_side, index, 1, 0)], 0)

    mine = [pair(0, labels, right_side)]
    mine[0], *later = lax.optimization_barrier((mine[0], labels, right_side))
    mine += [pair(q, *later) for q in range(1, depth)]
    near_first = send(mine[0], across)
    far_first = send(mine[-1], inside)
    near_next = send(mine[1], across)

    tables, factors, *state, near, far = call(
        start_kernel,
        (*mine, far_first, tensor_table, bounds),
        (tables, factors, field, cross_links, inplane_links, reaction, rest, field, plane, plane),
        0,
        LIMITS[0],
        10**8,
        halves,
        smem_count=2,
    )
    far_second = send(far, inside)
    near_second = send(near, across)

    *state, far, summed, half = call(
        middle_kernel,
        (*state, tables, factors, mine[0], far_second, near_first),
        tuple(array(*s.shape) for s in state) + (plane, inner, array(*halves[0].shape)),
        6,
        LIMITS[1],
        10**8,
        halves[1:],
    )
    far_third = send(far, inside)
    first, cross_links, inplane_links, reaction, rest, second = state
    first, second, rest, cross_links, _, solved = call(
        late_kernel,
        (first, second, rest, cross_links, half, inplane_links, reaction, factors, tables, near_next, summed),
        (field, field, array(*rest.shape), array(*cross_links.shape), array(*half.shape), block),
        5,
        LIMITS[2],
        10**8,
        [pltpu.VMEM((1, rows, columns), jnp.float32), pltpu.SemaphoreType.DMA((depth,))],
        kept=5,
    )
    links = (cross_links, inplane_links, reaction, factors)
    *_, residual, squares = call(
        last_kernel,
        (first, second, rest, *links, near_second, far_third),
        (field, field, array(*rest.shape), block, array(count, LANES)),
        3,
        LIMITS[3],
        10**8,
        [pltpu.SemaphoreType.DMA((depth, tiles))],
        kept=3,
    )
    gathered = lax.all_to_all(squares, "gz", 0, 0, tiled=True)
    return solved, residual, jnp.sqrt(jnp.sum(gathered[:, 0])).reshape(1)


def solution(mesh):
    whole = P(("groups", "gz"), None, None)
    return jax.shard_map(
        per_device,
        mesh=mesh,
        in_specs=(whole, P("groups", None), P("groups"), whole),
        out_specs=(whole, whole, P("groups")),
        check_vma=False,
    )
```

```python
import jax
import jax.numpy as jnp
from jax import lax
from jax.experimental import pallas as pl
from jax.experimental.pallas import tpu as pltpu
from jax.sharding import PartitionSpec as P


ITERS = 3
PHASES = 8
LANES = 128
SUB = 8
PAD = 8
BELOW = 8
RIM = 16
RIM_BELOW = 24
HALO = 2
OPERATOR_UNROLL = 16
LIMITS = (9, 5, 5, 5)

steps = (
    (1, 0, 0),
    (0, 1, 0),
    (0, 0, 1),
    (1, 1, 0),
    (1, -1, 0),
    (1, 0, 1),
    (1, 0, -1),
    (0, 1, 1),
    (0, 1, -1),
)
cross = [d for d, step in enumerate(steps) if step[0]]
inplane = [d for d, step in enumerate(steps) if not step[0]]


def slots(directions):
    order = [(d, 0) for d in directions] + [(d, 1) for d in directions if steps[d][2]]
    return {key: k for k, key in enumerate(order)}


cross_slots, inplane_slots = slots(cross), slots(inplane)


def splat(value):
    return jnp.full((SUB, LANES), value, jnp.float32)


def chebyshev(bounds_ref):
    lower, upper = splat(bounds_ref[0]), splat(bounds_ref[1])
    centre = (upper + lower) / 2.0
    half = (upper - lower) / 2.0
    sigma = centre / half
    rho = 1.0 / sigma
    factors = []
    for _ in range(ITERS):
        rho_new = 1.0 / (2.0 * sigma - rho)
        factors.append((rho_new * rho, 2.0 * rho_new / half))
        rho = rho_new
    return 1.0 / centre, factors


def each_block(rows, body, carry=0, unroll=None):
    count = rows // SUB
    unroll = min(unroll or 32, count)

    def step(k, carry):
        return body(pl.multiple_of(k * SUB, SUB), carry)

    carry = lax.fori_loop(0, count - count % unroll, step, carry, unroll=unroll)
    for k in range(count - count % unroll, count):
        carry = body(k * SUB, carry)
    return carry


def lane_shifted(values, dz, edge):
    lane = lax.broadcasted_iota(jnp.int32, (SUB, LANES), 1)
    turned = [pltpu.roll(value, LANES - 1 if dz == 1 else 1, 1) for value in values]
    if dz == 1:
        beyond = turned[1:] + [edge]
        return [jnp.where(lane == LANES - 1, b, t) for t, b in zip(turned, beyond)]
    beyond = [edge] + turned[:-1]
    return [jnp.where(lane == 0, b, t) for t, b in zip(turned, beyond)]


def put_field(field, plane, row, values):
    zero = splat(0.0)
    for variant, dz in ((0, 0), (1, 1), (2, -1)):
        shifted = lane_shifted(values, dz, zero) if dz else values
        for c, value in enumerate(shifted):
            field[plane, c, variant, pl.ds(row + PAD, SUB), :] = value


def field_rims(field, plane, tiles, rows):
    for variant in range(3):
        for c in range(tiles):
            field[plane, c, variant, pl.ds(0, PAD), :] = splat(0.0)
            field[plane, c, variant, pl.ds(rows + PAD, PAD), :] = splat(0.0)


def tile(ref, plane, c, row):
    return ref[plane, pl.ds(row, SUB), pl.ds(c * LANES, LANES)]


def label_of(ref):
    return lambda c, row: tile(ref, 0, c, row).astype(jnp.int32)


def put_tile(ref, plane, c, row, value):
    ref[plane, pl.ds(row, SUB), pl.ds(c * LANES, LANES)] = value


def put_tables(tables_ref, table_ref, flip):
    turn = jnp.where(splat(flip.astype(jnp.float32)) > 0.5, -0.5, 0.5)
    for phase in range(PHASES):
        k = [splat(table_ref[phase, column]) for column in range(7)]
        size = [jnp.abs(value) for value in k]
        values = (
            0.5 * (k[0] - size[3] - size[4]),
            turn * k[3],
            turn * k[4],
            0.5 * (k[1] - size[3] - size[5]),
            0.5 * (k[2] - size[4] - size[5]),
            0.5 * k[5],
            k[6],
        )
        for place, value in enumerate(values):
            tables_ref[phase, place] = value


def put_factors(factors_ref, bounds_ref):
    inverse, factors = chebyshev(bounds_ref)
    for k, value in enumerate([inverse] + [value for pair in factors for value in pair]):
        factors_ref[k] = value


def get_factors(factors_ref):
    pairs = [(factors_ref[1 + 2 * k], factors_ref[2 + 2 * k]) for k in range(ITERS)]
    return factors_ref[0], pairs


class Half:
    def __init__(self, tables_ref, refs, tiles, rows, clean=True):
        self.refs, self.tiles, self.rows = refs, tiles, rows
        self.tables = [
            ([tables_ref[phase, k] for k in range(3)], [tables_ref[phase, k] for k in range(3, 7)])
            for phase in range(PHASES)
        ]
        for ref, slots_of in zip(refs, (cross_slots, inplane_slots)):
            for slot in range(ref.shape[0] if clean else 0):
                for k in range(len(slots_of)):
                    for c in range(tiles):
                        for start in (0, SUB, rows + RIM, rows + RIM + SUB):
                            ref[slot, c, k, pl.ds(start, SUB), :] = splat(0.0)

    def fill(self, slot, read, mask=None, reaction=None):
        for group in range(2 if reaction else 1):
            tables = [t[group] for t in self.tables]
            if mask is not None:
                tables = [[mask * value for value in t] for t in tables]
            ref, at = (self.refs[1], 0) if group else (self.refs[0], slot)
            places = inplane_slots if group else cross_slots

            def body(row, carry):
                found = {}
                for c in range(self.tiles):
                    label = read(c, row)
                    bits = [(label & (1 << b)) != 0 for b in range(3)]
                    looked = []
                    for column in range(len(tables[0])):
                        level = [t[column] for t in tables]
                        for bit in bits:
                            level = [jnp.where(bit, b, a) for a, b in zip(level[::2], level[1::2])]
                        looked.append(level[0])
                    if group == 0:
                        values = {0: looked[0]}
                        signed = zip((3, 5), looked[1:])
                    else:
                        values = {1: looked[0], 2: looked[1]}
                        signed = [(7, looked[2])]
                        reaction[0][reaction[1], c, pl.ds(row, SUB), :] = looked[3]
                    for d, value in signed:
                        values[d] = jnp.maximum(value, 0.0)
                        values[d + 1] = jnp.maximum(-value, 0.0)
                    for d, value in values.items():
                        ref[at, c, places[d, 0], pl.ds(row + RIM, SUB), :] = value
                        found.setdefault(d, []).append(value)
                for d, values in found.items():
                    if steps[d][2]:
                        for c, value in enumerate(lane_shifted(values, steps[d][2], splat(0.0))):
                            ref[at, c, places[d, 1], pl.ds(row + RIM, SUB), :] = value
                return carry

            each_block(self.rows, body)

    def link(self, slot, other, out, at):
        directions, places = (cross, cross_slots) if other is not None else (inplane, inplane_slots)
        ref = self.refs[0 if other is not None else 1]
        slot, other = (slot, other) if other is not None else (0, 0)

        def body(row, carry):
            for d in directions:
                _, dy, dz = steps[d]
                near = pl.ds(row + RIM - PAD, SUB)
                far = pl.ds(row + RIM - PAD + dy, SUB)
                ahead = [ref[other, c, places[d, 1 if dz else 0], far, :] for c in range(self.tiles)]
                values = [ref[slot, c, places[d, 0], near, :] + ahead[c] for c in range(self.tiles)]
                for c, value in enumerate(values):
                    out[at, c, places[d, 0], pl.ds(row, SUB), :] = value
                if dz:
                    edge = ref[other, 0 if dz == 1 else self.tiles - 1, places[d, 0], far, :]
                    for c, value in enumerate(lane_shifted(values, -dz, edge)):
                        out[at, c, places[d, 1], pl.ds(row, SUB), :] = value
            return carry

        each_block(self.rows + 2 * PAD, body, unroll=17)


def run_operator(field, links, planes, device, use, parts={}, carry=0):
    cross_ref, inplane_ref, reaction_ref = links

    def body(row, carry):
        held = {}

        def value(q, c, dy, dz):
            key = (q, c, dy, dz)
            if key not in held:
                held[key] = field[q + HALO, c, dz % 3, pl.ds(row + PAD + dy, SUB), :]
            return held[key]

        def image(q, c):
            here = value(q, c, 0, 0)
            wanted = parts.get(q, (-1, 0, 1))
            sums = [reaction_ref[q + 1, c, pl.ds(row, SUB), :] * here] if 0 in wanted else []
            for d, (dx, dy, dz) in enumerate(steps):
                places = cross_slots if dx else inplane_slots
                ref, base = (cross_ref, HALO) if dx else (inplane_ref, 1)
                for sign in (1, -1):
                    if sign * dx not in wanted:
                        continue
                    if sign == 1:
                        link = ref[q + base, c, places[d, 0], pl.ds(row + PAD, SUB), :]
                    else:
                        key = places[d, 1 if dz else 0]
                        link = ref[q + base - dx, c, key, pl.ds(row + PAD - dy, SUB), :]
                    term = link * (here - value(q + sign * dx, c, sign * dy, sign * dz))
                    sums = sums[1:] + [sums[0] + term] if len(sums) == 3 else sums + [term]
            return sums[0] + (sums[1] + sums[2])

        for q in planes:
            images = [image(q, c) for c in range(device.tiles)]
            carry = use(q, row, images, [value(q, c, 0, 0) for c in range(device.tiles)], carry)
        return carry

    return each_block(device.rows, body, carry, unroll=OPERATOR_UNROLL)


class Device:
    def __init__(self, shape):
        self.depth, self.rows, self.tiles = shape[0], shape[1], shape[2] // LANES
        self.place, self.count = lax.axis_index("gz"), lax.axis_size("gz")
        self.flip = self.place % 2
        joined = jnp.logical_and(self.place > 0, self.place < self.count - 1)
        self.joined = splat(joined.astype(jnp.float32))

    def own(self, q):
        return jnp.where(self.flip == 1, self.depth - 1 - q, q)


class Solve:
    def __init__(self, device, refs, factors, right=None):
        self.device, self.factors, self.right = device, factors, right
        self.first, self.second, *self.links, self.rest = refs

    def advance(self, iteration, planes, direct=(), parts={}, copies={}, keep=None):
        device, rest_ref = self.device, self.rest
        old, new = (self.first, self.second) if iteration == 0 else (self.second, self.first)
        ahead, behind = self.factors[iteration]
        if iteration == 2:
            old, new = new, old
        for q in direct:
            if q < 0:
                field_rims(new, q + HALO, device.tiles, device.rows)

        def use(q, row, images, here, carry):
            block = pl.ds(row, SUB)
            if self.right and iteration == 0 and q < 0:
                before = [self.right(q, c, row) for c in range(device.tiles)]
            else:
                before = [rest_ref[q + 1, c, block, :] for c in range(device.tiles)]
            rest = [b - image for b, image in zip(before, images)]
            if q < 0:
                rest = [device.joined * r for r in rest]
            for c, r in enumerate(rest):
                rest_ref[q + 1, c, block, :] = r
            if q in direct:
                values = [ahead * h + behind * r for h, r in zip(here, rest)]
                if q in copies:
                    for c, v in enumerate(values):
                        put_tile(copies[q], 0, c, row, v)
                if keep and 0 <= q:
                    for c, (h, v) in enumerate(zip(here, values)):
                        keep(q, c, row, new[q + HALO, c, 0, pl.ds(row + PAD, SUB), :] + h + v)
                put_field(new, q + HALO, row, values)
            return carry

        run_operator(old, self.links, planes, device, use, parts)

    def receive(self, field, q, read):
        field_rims(field, q + HALO, self.device.tiles, self.device.rows)

        def body(row, carry):
            put_field(field, q + HALO, row, [read(c, row) for c in range(self.device.tiles)])
            return carry

        each_block(self.device.rows, body)


def start_kernel(*refs):
    *pairs, table_ref, bounds_ref, tables_ref, factors_ref = refs[:9]
    first_ref, cross_ref, inplane_ref, reaction_ref, rest_ref, second_ref, near_ref, far_ref, own_ref = refs[9:18]
    halves = refs[18:]
    device = Device((len(pairs) - 1,) + pairs[0].shape[1:])
    depth, rows, tiles = device.depth, device.rows, device.tiles
    put_factors(factors_ref, bounds_ref)
    inverse, factors = get_factors(factors_ref)
    put_tables(tables_ref, table_ref, device.flip)
    half = Half(tables_ref, halves, tiles, rows)

    for q, pair_ref in enumerate(pairs):
        field_rims(first_ref, q + HALO, tiles, rows)
        field_rims(second_ref, q + HALO, tiles, rows)

        def body(row, carry):
            values = [tile(pair_ref, 1, c, row) for c in range(tiles)]
            if q == 0:
                for c in range(tiles):
                    put_tile(own_ref, 0, c, row, tile(pair_ref, 0, c, row))
            if q < depth:
                for c, value in enumerate(values):
                    rest_ref[q + 1, c, pl.ds(row, SUB), :] = value
            put_field(first_ref, q + HALO, row, [value * inverse for value in values])
            return carry

        each_block(rows, body)
        half.fill(q % 2, label_of(pair_ref), None, (reaction_ref, q + 1) if q < depth else None)
        if q:
            half.link((q - 1) % 2, q % 2, cross_ref, q - 1 + HALO)
        if q < depth:
            half.link(q % 2, None, inplane_ref, q + 1)

    solve = Solve(device, (first_ref, second_ref, cross_ref, inplane_ref, reaction_ref, rest_ref), factors)
    solve.advance(0, range(depth), range(1, depth), parts={0: (0, 1)}, copies={1: near_ref, depth - 1: far_ref})


def middle_kernel(*refs):
    tables_ref, factors_ref, own_ref, far_second_ref, near_ref = refs[6:11]
    first_ref, cross_ref, inplane_ref, reaction_ref, rest_ref, second_ref, far_ref, sum_ref, *halves = refs[11:]
    depth = rest_ref.shape[0] - 1
    device = Device((depth,) + near_ref.shape[1:])
    inverse, factors = get_factors(factors_ref)
    half = Half(tables_ref, halves, device.tiles, device.rows)
    half.fill(0, label_of(own_ref))
    half.fill(1, label_of(near_ref), device.joined, (reaction_ref, 0))
    half.link(1, None, inplane_ref, 0)
    half.link(1, 0, cross_ref, HALO - 1)

    def right(q, c, row):
        return tile(near_ref, 1, c, row)

    def keep(q, c, row, value):
        put_tile(sum_ref, q - 1, c, row, value)

    solve = Solve(device, (first_ref, second_ref, cross_ref, inplane_ref, reaction_ref, rest_ref), factors, right)
    solve.receive(first_ref, -1, lambda c, row: tile(near_ref, 1, c, row) * inverse)
    solve.advance(0, [-1, 0], [0], parts={-1: (0, 1), 0: (-1,)})
    solve.receive(second_ref, depth, lambda c, row: tile(far_second_ref, 0, c, row))
    solve.advance(1, range(depth), range(1, depth), parts={0: (0, 1)}, copies={depth - 1: far_ref}, keep=keep)
    solve.advance(2, range(1, depth), parts={1: (0, 1), depth - 1: (-1, 0)})


def late_kernel(*refs):
    inplane_ref, reaction_ref, factors_ref, tables_ref, near_ref, sum_ref = refs[5:11]
    first_ref, second_ref, rest_ref, cross_ref, half_ref, solution_ref, ready_ref, sems = refs[11:]
    device = Device(solution_ref.shape)
    depth = device.depth
    inverse, factors = get_factors(factors_ref)
    copies = [
        pltpu.make_async_copy(
            sum_ref.at[q - 1] if q else ready_ref.at[0], solution_ref.at[device.own(q)], sems.at[q]
        )
        for q in range(depth)
    ]
    for copy in copies[1:]:
        copy.start()
    half = Half(tables_ref, (half_ref,), device.tiles, device.rows, clean=False)
    half.fill(0, label_of(near_ref), device.joined)
    half.link(0, 1, cross_ref, HALO - 2)

    def keep(q, c, row, value):
        put_tile(ready_ref, q, c, row, value)

    solve = Solve(device, (first_ref, second_ref, cross_ref, inplane_ref, reaction_ref, rest_ref), factors)
    solve.receive(first_ref, -2, lambda c, row: tile(near_ref, 1, c, row) * inverse)
    solve.advance(0, [-1], [-1], parts={-1: (-1,)})
    solve.advance(1, [-1, 0], [0], parts={-1: (0, 1), 0: (-1,)}, keep=keep)
    copies[0].start()
    solve.advance(2, [0, 1], parts={0: (0, 1), 1: (-1,)})
    for copy in copies:
        copy.wait()


def last_kernel(*refs):
    *links, factors_ref, near_second_ref, far_third_ref = refs[3:9]
    first_ref, second_ref, rest_ref, residual_ref, squares_ref, sems = refs[9:]
    device = Device(residual_ref.shape)
    depth = device.depth
    copies = {
        q: [
            pltpu.make_async_copy(
                rest_ref.at[q + 1, c],
                residual_ref.at[device.own(q), :, pl.ds(c * LANES, LANES)],
                sems.at[q, c],
            )
            for c in range(device.tiles)
        ]
        for q in range(depth)
    }
    for q in range(1, depth - 1):
        for copy in copies[q]:
            copy.start()
    _, factors = get_factors(factors_ref)
    solve = Solve(device, (first_ref, second_ref, *links, rest_ref), factors)
    solve.receive(first_ref, depth, lambda c, row: tile(far_third_ref, 0, c, row))
    solve.receive(second_ref, -2, lambda c, row: tile(near_second_ref, 0, c, row))
    solve.advance(1, [-1], [-1], parts={-1: (-1,)})

    def use(q, row, images, here, carry):
        for c, image in enumerate(images):
            for plane in range(depth - 1) if q == 0 else [q]:
                rest = rest_ref[plane + 1, c, pl.ds(row, SUB), :]
                if plane == q:
                    rest = rest - image
                    rest_ref[plane + 1, c, pl.ds(row, SUB), :] = rest
                carry = carry + rest * rest
        return carry

    ends = {0: (-1,), depth - 1: (1,)}
    total = run_operator(first_ref, links, list(ends), device, use, ends, splat(0.0))
    for q in ends:
        for copy in copies[q]:
            copy.start()
    squares_ref[...] = jnp.broadcast_to(jnp.sum(total), squares_ref.shape)
    for q in range(depth):
        for copy in copies[q]:
            copy.wait()


def per_device(labels, tensor_table, bounds, right_side):
    depth, rows, columns = labels.shape
    if depth != 2 * HALO or columns % LANES or rows % SUB:
        raise ValueError("unsupported block")
    tiles = columns // LANES
    count = lax.axis_size("gz")
    odd = lax.axis_index("gz") % 2

    vmem = pl.BlockSpec(memory_space=pltpu.VMEM)
    smem = pl.BlockSpec(memory_space=pltpu.SMEM)
    hbm = pl.BlockSpec(memory_space=pltpu.HBM)

    def array(*shape):
        return jax.ShapeDtypeStruct(shape, jnp.float32)

    below = rows + PAD + BELOW
    field = array(depth + HALO + 1, tiles, 3, below, LANES)
    cross_links = array(depth + HALO, tiles, len(cross_slots), below, LANES)
    inplane_links = array(depth + 1, tiles, len(inplane_slots), below, LANES)
    reaction = rest = array(depth + 1, tiles, rows, LANES)
    inner = array(depth - 1, rows, columns)
    plane = array(1, rows, columns)
    block = array(depth, rows, columns)
    tables, factors = array(PHASES, 7, SUB, LANES), array(1 + 2 * ITERS, SUB, LANES)
    halves = [
        pltpu.VMEM((planes, tiles, len(places), rows + RIM + RIM_BELOW, LANES), jnp.float32)
        for planes, places in ((2, cross_slots), (1, inplane_slots))
    ]

    def call(kernel, arguments, out_shape, aliased, limit, flops, scratch=(), smem_count=0, kept=None):
        return pl.pallas_call(
            kernel,
            out_shape=out_shape,
            in_specs=[vmem] * (len(arguments) - smem_count) + [smem] * smem_count,
            out_specs=[hbm if k == kept else vmem for k in range(len(out_shape))],
            scratch_shapes=list(scratch),
            input_output_aliases={k: k for k in range(aliased)},
            compiler_params=pltpu.CompilerParams(vmem_limit_bytes=limit << 20),
            cost_estimate=pl.CostEstimate(flops=flops, bytes_accessed=1 << 20, transcendentals=0),
        )(*arguments)

    inside = [(i, i ^ 1) for i in range(count)]
    across = [(i, i + 1) for i in range(1, count - 1, 2)]
    across += [(j, i) for i, j in across]

    def send(array, pairs):
        return lax.ppermute(array, "gz", pairs)

    def pair(q, labels, right_side):
        index = jnp.where(odd == 1, depth - 1 - q, q)
        own_labels = lax.dynamic_slice_in_dim(labels, index, 1, 0).astype(jnp.float32)
        return jnp.concatenate([own_labels, lax.dynamic_slice_in_dim(right_side, index, 1, 0)], 0)

    mine = [pair(0, labels, right_side)]
    mine[0], *later = lax.optimization_barrier((mine[0], labels, right_side))
    mine += [pair(q, *later) for q in range(1, depth)]
    near_first = send(mine[0], across)
    far_first = send(mine[-1], inside)
    near_next = send(mine[1], across)

    tables, factors, *state, near, far, own_labels = call(
        start_kernel,
        (*mine, far_first, tensor_table, bounds),
        (tables, factors, field, cross_links, inplane_links, reaction, rest, field, plane, plane, plane),
        0,
        LIMITS[0],
        10**8,
        halves,
        smem_count=2,
    )
    far_second = send(far, inside)
    near_second = send(near, across)

    *state, far, summed, half = call(
        middle_kernel,
        (*state, tables, factors, own_labels, far_second, near_first),
        tuple(array(*s.shape) for s in state) + (plane, inner, array(*halves[0].shape)),
        6,
        LIMITS[1],
        10**8,
        halves[1:],
    )
    far_third = send(far, inside)
    first, cross_links, inplane_links, reaction, rest, second = state
    first, second, rest, cross_links, _, solved = call(
        late_kernel,
        (first, second, rest, cross_links, half, inplane_links, reaction, factors, tables, near_next, summed),
        (field, field, array(*rest.shape), array(*cross_links.shape), array(*half.shape), block),
        5,
        LIMITS[2],
        10**8,
        [pltpu.VMEM((1, rows, columns), jnp.float32), pltpu.SemaphoreType.DMA((depth,))],
        kept=5,
    )
    links = (cross_links, inplane_links, reaction, factors)
    *_, residual, squares = call(
        last_kernel,
        (first, second, rest, *links, near_second, far_third),
        (field, field, array(*rest.shape), block, array(count, LANES)),
        3,
        LIMITS[3],
        10**8,
        [pltpu.SemaphoreType.DMA((depth, tiles))],
        kept=3,
    )
    gathered = lax.all_to_all(squares, "gz", 0, 0, tiled=True)
    return solved, residual, jnp.sqrt(jnp.sum(gathered[:, 0])).reshape(1)


def solution(mesh):
    whole = P(("groups", "gz"), None, None)
    return jax.shard_map(
        per_device,
        mesh=mesh,
        in_specs=(whole, P("groups", None), P("groups"), whole),
        out_specs=(whole, whole, P("groups")),
        check_vma=False,
    )
```
